512 devices in a mesh: dom: 64 (over x, y, core), sub: 8 (over z).
Axes of the slice: x: 4, y: 8, z: 8, core: 2. Of those that a mesh axis runs over, the one named last changes fastest.
Arguments:
- inv_interior: bfloat16 [512, 80000], P(('dom', 'sub'))
- couple_if: bfloat16 [512, 160000], P(('dom', 'sub')), may hold values from -0.625 to 0.625
- couple_fi: bfloat16 [512, 160000], P(('dom', 'sub')), may hold values from -0.625 to 0.625
- face_face: bfloat16 [512, 320000], P(('dom', 'sub'))
- load_interior: float32 [4096, 100], P(('dom', 'sub')), may hold values from -6 to 6
- load_face: float32 [4096, 200], P(('dom', 'sub')), may hold values from -24 to 24
- jacobi_inverse: bfloat16 [12288, 2500], P(('dom', 'sub'))
- slot_face: int32 [4096, 4], P(('dom', 'sub')), may hold values from 0 to 24, as said below
- send_slot: int32 [512, 4, 2], P(('dom', 'sub')), may hold values from 0 to 32, as said below
- recv_face: int32 [512, 4, 2], P(('dom', 'sub')), may hold values from 0 to 24, as said below
- partner_sub: int32 [512, 8], P(('dom', 'sub')), may hold values from 0 to 7, as said below
- elem_count: int32 [512], P(('dom', 'sub')), may hold values from 4 to 8, as said below
Outputs:
- face_trace: float32 [12288, 50], P(('dom', 'sub'))
- interior_state: float32 [4096, 100], P(('dom', 'sub'))
- face_blocks: bfloat16 [12288, 2500], P(('dom', 'sub'))
The draws below stay inside these ranges and needn't reach their ends.
Inputs may be any that keep to these rules, and one draw needn't show every extreme that they name: `slot_face`: for each element face: the index of its face among its own device's faces when that device owns it, else 24. Faces of elements at or past elem_count are 24. Every element face of a live element lies either here or in exactly one holder list; a face is met by one or two element faces. `send_slot`: holder lists of each device and group: element face positions 4 * e + k of this device, live rows first, 32 for empty rows; at most 2 live rows a list, and one list of some device has exactly 2. Row r matches row r of the owner's list, the owner of group g lying off(g) positions lower along dom, cyclically. `recv_face`: owner lists of each device and group: local face indices, live rows first, 24 for empty rows; the live rows equal in number those of the matching holder list, whose device lies off(g) positions higher along dom for group g. `partner_sub`: entry g is the sub index of the device's holder for group g; entry 4 + g that of its owner for group g. For each dom index and group, owners and holders are paired one to one by sub index; in group 0 no device is paired with itself. `elem_count`: live elements of each device; some device has 8.
All inputs are finite; a program needn't handle non-finite values.
Results may differ from the reference program's by a relative error of at most 0.0051.
Values sent between devices are 32-bit elements; how exact they have to be, the bound alone decides.
A program may use at most 64 MiB of HBM per device.

```python
import jax
import jax.numpy as jnp
from jax import lax

INTERIOR = 100
FACE_DOF = 50
GROUPS = 4
SWEEPS = 2
ELEM_DEV = 8
CAP = 2
FACE_DEV = 24
ELEMS = 4096
FACES = 12288
N_SUB = 8
DEVICES = 512


def dominant(key, count, order, low, high, spread):
    key_diag, key_jitter = jax.random.split(key)
    diagonal = jnp.exp(jax.random.uniform(key_diag, (count, order), minval=jnp.log(low), maxval=jnp.log(high)))
    jitter = jax.random.normal(key_jitter, (count, order, order)) * (spread / order ** 0.5)
    return jitter + diagonal[:, :, None] * jnp.eye(order, dtype=jnp.float32)[None]


def draw_inv_interior(key, part):
    matrix = dominant(jax.random.fold_in(key, 11), ELEMS, INTERIOR, 0.5, 2.0, 0.4)
    return matrix.reshape(ELEMS // 8, 8 * INTERIOR * INTERIOR).astype(jnp.bfloat16)


def draw_face_face(key, part):
    matrix = dominant(jax.random.fold_in(key, 13), ELEMS, 4 * FACE_DOF, 3.0, 6.0, 1.2)
    return matrix.reshape(ELEMS // 8, 8 * 16 * FACE_DOF * FACE_DOF).astype(jnp.bfloat16)


def draw_jacobi_inverse(key, part):
    matrix = dominant(jax.random.fold_in(key, 17), FACES, FACE_DOF, 0.08, 0.15, 0.03)
    return matrix.reshape(FACES, FACE_DOF * FACE_DOF).astype(jnp.bfloat16)


def build_links(key):
    key = jax.random.fold_in(key, 97)
    key_turn, key_perm, key_count, key_star, key_elems, key_order = jax.random.split(key, 6)
    dom_total = DEVICES // N_SUB
    slot_span = 4 * ELEM_DEV
    device_ids = jnp.arange(DEVICES, dtype=jnp.int32)
    dom_ids = device_ids // N_SUB
    sub_ids = device_ids % N_SUB
    sub_range = jnp.arange(N_SUB, dtype=jnp.int32)
    group_ids = jnp.arange(GROUPS, dtype=jnp.int32)
    offsets = jnp.array([0, 1, dom_total // 2, dom_total - 1], dtype=jnp.int32)
    turn = jax.random.randint(key_turn, (dom_total,), 1, N_SUB)
    scores = jax.random.randint(key_perm, (dom_total, GROUPS, N_SUB), 0, 1 << 20) * N_SUB + sub_range
    sigma = jnp.argsort(scores, axis=-1).astype(jnp.int32)
    sigma = sigma.at[:, 0, :].set(((sub_range[None, :] + turn[:, None]) % N_SUB).astype(jnp.int32))
    inverse = jnp.argsort(sigma, axis=-1).astype(jnp.int32)
    holder_sub = sigma[dom_ids[:, None], group_ids[None, :], sub_ids[:, None]]
    owner_dom = (dom_ids[:, None] - offsets[None, :]) % dom_total
    owner_sub = inverse[owner_dom, group_ids[None, :], sub_ids[:, None]]
    owner_dev = owner_dom * N_SUB + owner_sub
    counts = jax.random.randint(key_count, (DEVICES, GROUPS), 0, CAP + 1)
    star_dev = jax.random.randint(key_star, (), 0, DEVICES)
    counts = jnp.where(device_ids[:, None] == star_dev, CAP, counts).astype(jnp.int32)
    incoming = counts[owner_dev, group_ids[None, :]]
    out_total = counts.sum(axis=1)
    in_total = incoming.sum(axis=1)
    lowest = jnp.maximum(jnp.maximum((out_total + in_total + 3) // 4, ELEM_DEV // 2), 1)
    alive = jax.random.randint(key_elems, (DEVICES,), lowest, ELEM_DEV + 1)
    alive = jnp.where(device_ids == (star_dev + DEVICES // 2) % DEVICES, ELEM_DEV, alive).astype(jnp.int32)
    live_slots = 4 * alive
    positions = jnp.arange(slot_span, dtype=jnp.int32)
    order_keys = (positions[None, :] >= live_slots[:, None]).astype(jnp.int32) * (1 << 24)
    order_keys = order_keys + jax.random.randint(key_order, (DEVICES, slot_span), 0, 1 << 12) * slot_span + positions[None, :]
    order = jnp.argsort(order_keys, axis=-1).astype(jnp.int32)
    rank = jnp.argsort(order, axis=-1).astype(jnp.int32)
    roles = jnp.broadcast_to(positions[None, :], (DEVICES, slot_span))
    after_out = roles - out_total[:, None]
    after_in = after_out - in_total[:, None]
    role_face = jnp.where(roles < out_total[:, None], roles, jnp.where(after_out < in_total[:, None], FACE_DEV, jnp.where(roles < live_slots[:, None], out_total[:, None] + after_in // 2, FACE_DEV)))
    slot_face = jnp.take_along_axis(role_face.astype(jnp.int32), rank, axis=1)
    lanes = jnp.arange(CAP, dtype=jnp.int32)
    start_out = jnp.cumsum(counts, axis=1) - counts
    recv_face = jnp.where(lanes[None, None, :] < counts[:, :, None], start_out[:, :, None] + lanes[None, None, :], FACE_DEV)
    start_in = jnp.cumsum(incoming, axis=1) - incoming
    in_roles = jnp.minimum(out_total[:, None, None] + start_in[:, :, None] + lanes[None, None, :], slot_span - 1)
    send_pos = jnp.take_along_axis(order, in_roles.reshape(DEVICES, GROUPS * CAP), axis=1).reshape(DEVICES, GROUPS, CAP)
    send_slot = jnp.where(lanes[None, None, :] < incoming[:, :, None], send_pos, slot_span)
    partner_sub = jnp.concatenate([holder_sub, owner_sub], axis=1)
    return (slot_face.reshape(ELEMS, 4).astype(jnp.int32), send_slot.astype(jnp.int32), recv_face.astype(jnp.int32), partner_sub.astype(jnp.int32), alive)


def draw_slot_face(key, part):
    return build_links(key)[0]


def draw_send_slot(key, part):
    return build_links(key)[1]


def draw_recv_face(key, part):
    return build_links(key)[2]


def draw_partner_sub(key, part):
    return build_links(key)[3]


def draw_elem_count(key, part):
    return build_links(key)[4]


def shard_levels(stream_key, dims, shards, low, high):
    level, own = 1.0, jax.random.fold_in(stream_key, 6)
    for dim, shards_of in shards:
        heights = jnp.exp(jax.random.uniform(jax.random.fold_in(own, dim), (shards_of,), jnp.float32, low / len(shards), high / len(shards)))
        level = level * jnp.repeat(heights, dims[dim] // shards_of).reshape([-1 if axis == dim else 1 for axis in range(len(dims))])
    return level


def scatter_about(rng, shape, deviation, limit, cuts=(), kind=jnp.bfloat16):
    values = deviation * jax.random.normal(rng, shape, jnp.float32)
    if cuts:
        values = values * shard_levels(rng, shape, cuts, -0.22, 0.18)
    return jnp.clip(values, -limit, limit).astype(kind)


def setup_inputs(seed: int = 0) -> dict:
    streams_of = jax.random.split(jax.random.key(seed), 13)
    inv_interior = draw_inv_interior(jax.random.fold_in(streams_of[12], 71), 0)
    couple_if = scatter_about(streams_of[1], (ELEMS // 8, 8 * INTERIOR * 4 * FACE_DOF), INTERIOR ** -0.5, 0.625, ((0, 512),))
    couple_fi = scatter_about(streams_of[2], (ELEMS // 8, 8 * 4 * FACE_DOF * INTERIOR), INTERIOR ** -0.5, 0.625, ((0, 512),))
    face_face = draw_face_face(jax.random.fold_in(streams_of[12], 71), 0)
    load_interior = scatter_about(streams_of[4], (ELEMS, INTERIOR), 1.0, 6.0, ((0, 512),), jnp.float32)
    load_face = scatter_about(streams_of[5], (ELEMS, 4 * FACE_DOF), 4.0, 24.0, ((0, 512),), jnp.float32)
    jacobi_inverse = draw_jacobi_inverse(jax.random.fold_in(streams_of[12], 71), 0)
    slot_face = draw_slot_face(jax.random.fold_in(streams_of[12], 71), 0)
    send_slot = draw_send_slot(jax.random.fold_in(streams_of[12], 71), 0)
    recv_face = draw_recv_face(jax.random.fold_in(streams_of[12], 71), 0)
    partner_sub = draw_partner_sub(jax.random.fold_in(streams_of[12], 71), 0)
    elem_count = draw_elem_count(jax.random.fold_in(streams_of[12], 71), 0)
    return {"inv_interior": inv_interior, "couple_if": couple_if, "couple_fi": couple_fi, "face_face": face_face, "load_interior": load_interior, "load_face": load_face, "jacobi_inverse": jacobi_inverse, "slot_face": slot_face, "send_slot": send_slot, "recv_face": recv_face, "partner_sub": partner_sub, "elem_count": elem_count}


HIGH = lax.Precision.HIGHEST


def group_offset(group_index, dom_total):
    return [0, 1, dom_total // 2, dom_total - 1][group_index]


def slot_maps(slot_face, send_slot, recv_face, partner_sub):
    slot_span = 4 * ELEM_DEV
    dom_total = DEVICES // N_SUB
    dummy_face = DEVICES * FACE_DEV
    spill_index = DEVICES * slot_span
    device_ids = jnp.arange(DEVICES, dtype=jnp.int32)
    dom_ids = device_ids // N_SUB
    local_face = slot_face.reshape(DEVICES, slot_span)
    local_ids = jnp.where(local_face < FACE_DEV, device_ids[:, None] * FACE_DEV + local_face, dummy_face).reshape(-1).astype(jnp.int32)
    scatter_ids = local_ids
    gather_ids = local_ids
    for group_index in range(GROUPS):
        offset = group_offset(group_index, dom_total)
        owner_dev = (((dom_ids - offset) % dom_total) * N_SUB + partner_sub[:, GROUPS + group_index]).astype(jnp.int32)
        owner_face = recv_face[owner_dev, group_index, :]
        own_slot = send_slot[:, group_index, :]
        usable = (own_slot < slot_span) & (owner_face < FACE_DEV)
        target = jnp.where(usable, device_ids[:, None] * slot_span + own_slot, spill_index).reshape(-1).astype(jnp.int32)
        face_ids = (owner_dev[:, None] * FACE_DEV + owner_face).reshape(-1).astype(jnp.int32)
        scatter_ids = scatter_ids.at[target].set(face_ids, mode="drop")
        holder_dev = (((dom_ids + offset) % dom_total) * N_SUB + partner_sub[:, group_index]).astype(jnp.int32)
        holder_slot = send_slot[holder_dev, group_index, :]
        face_here = recv_face[:, group_index, :]
        usable = (holder_slot < slot_span) & (face_here < FACE_DEV)
        target = jnp.where(usable, holder_dev[:, None] * slot_span + holder_slot, spill_index).reshape(-1).astype(jnp.int32)
        face_ids = (device_ids[:, None] * FACE_DEV + face_here).reshape(-1).astype(jnp.int32)
        gather_ids = gather_ids.at[target].set(face_ids, mode="drop")
    return scatter_ids, gather_ids


def local_section(pieces):
    inverse, couple_in, couple_out, face_block, load_in, load_out, living = pieces
    interior_map = jnp.einsum("eij,ejk->eik", inverse.astype(jnp.float32), couple_in.astype(jnp.float32), precision=HIGH).astype(jnp.bfloat16)
    interior_load = jnp.einsum("eij,ej->ei", inverse.astype(jnp.float32), load_in, precision=HIGH)
    product = jnp.einsum("eij,ejk->eik", couple_out.astype(jnp.float32), interior_map.astype(jnp.float32), precision=HIGH)
    condensed = ((face_block.astype(jnp.float32) - product) * living[:, None, None]).astype(jnp.bfloat16)
    face_load = (load_out - jnp.einsum("eij,ej->ei", couple_out.astype(jnp.float32), interior_load, precision=HIGH)) * living[:, None]
    return interior_map, interior_load, condensed, face_load


def multiply_blocks(pieces):
    condensed, elem_traces = pieces
    return jnp.einsum("eij,ej->ei", condensed.astype(jnp.float32), elem_traces, precision=HIGH)


def back_solve(pieces):
    interior_map, interior_load, elem_traces, living = pieces
    images = jnp.einsum("eij,ej->ei", interior_map.astype(jnp.float32), elem_traces, precision=HIGH)
    return (interior_load - images) * living[:, None]


def reference(inv_interior, couple_if, couple_fi, face_face, load_interior, load_face, jacobi_inverse, slot_face, send_slot, recv_face, partner_sub, elem_count):
    slot_total = DEVICES * ELEM_DEV * 4
    face_total = DEVICES * FACE_DEV
    width_face = 4 * FACE_DOF
    living = (jnp.arange(ELEM_DEV, dtype=jnp.int32)[None, :] < elem_count[:, None]).astype(jnp.float32)
    stacked = (inv_interior.reshape(DEVICES, ELEM_DEV, INTERIOR, INTERIOR),
               couple_if.reshape(DEVICES, ELEM_DEV, INTERIOR, width_face),
               couple_fi.reshape(DEVICES, ELEM_DEV, width_face, INTERIOR),
               face_face.reshape(DEVICES, ELEM_DEV, width_face, width_face),
               load_interior.reshape(DEVICES, ELEM_DEV, INTERIOR),
               load_face.reshape(DEVICES, ELEM_DEV, width_face),
               living)
    interior_map, interior_load, condensed, face_load = lax.map(local_section, stacked)
    scatter_ids, gather_ids = slot_maps(slot_face, send_slot, recv_face, partner_sub)

    def assemble(values):
        return jax.ops.segment_sum(values, scatter_ids, num_segments=face_total + 1)[:face_total]

    def distribute(traces):
        padded = jnp.concatenate([traces, jnp.zeros((1, FACE_DOF), jnp.float32)], axis=0)
        return padded[gather_ids].reshape(DEVICES, ELEM_DEV, width_face)

    shaped = condensed.reshape(DEVICES * ELEM_DEV, 4, FACE_DOF, 4, FACE_DOF)
    blocks = jnp.stack([shaped[:, side_index, :, side_index, :] for side_index in range(4)], axis=1)
    blocks = blocks.reshape(slot_total, FACE_DOF * FACE_DOF).astype(jnp.float32)
    face_blocks = assemble(blocks)
    face_rhs = assemble(face_load.reshape(slot_total, FACE_DOF))
    inverse = jacobi_inverse.astype(jnp.float32).reshape(face_total, FACE_DOF, FACE_DOF)
    traces = jnp.einsum("fij,fj->fi", inverse, face_rhs, precision=HIGH)
    for sweep_index in range(SWEEPS):
        images = lax.map(multiply_blocks, (condensed, distribute(traces)))
        residual = face_rhs - assemble(images.reshape(slot_total, FACE_DOF))
        traces = traces + jnp.einsum("fij,fj->fi", inverse, residual, precision=HIGH)
    interior_state = lax.map(back_solve, (interior_map, interior_load, distribute(traces), living))
    return traces, interior_state.reshape(DEVICES * ELEM_DEV, INTERIOR), face_blocks.astype(jnp.bfloat16)
```

```python
import functools

import jax
import jax.numpy as jnp
from jax import lax
from jax.experimental import pallas as pl
from jax.experimental.pallas import tpu as pltpu
from jax.sharding import PartitionSpec as P

HIGH = lax.Precision.HIGHEST
SWEEPS = 2
GROUPS = 4
DOF = 50
CHUNKS = 5
F32, BF16 = jnp.float32, jnp.bfloat16


def group_offset(group, doms):
    return [0, 1, doms // 2, doms - 1][group]


def split_dot(left, right):
    high = right.astype(BF16)
    low = (right - high.astype(F32)).astype(BF16)
    return jnp.dot(left, high, preferred_element_type=F32) + jnp.dot(
        left, low, preferred_element_type=F32
    )


def exchange_kernel(
    doms, subs,
    select_ref, partner_ref, condensed_ref, imap_ref, iload_ref, fload_ref, jac_ref, blocks_ref, living_ref,
    trace_ref, state_ref, faces_ref,
    jflat, jrows, sbuf, rbuf, sbig, rbig, send_sem, recv_sem, bsend_sem, brecv_sem,
):
    dom, sub = lax.axis_index("dom"), lax.axis_index("sub")
    offsets = [group_offset(g, doms) for g in range(GROUPS)]
    for phase in range(6):
        rbuf[phase] = jnp.zeros(rbuf.shape[1:], F32)
    barrier = pltpu.get_barrier_semaphore()

    def greet(step, carry):
        for g in range(GROUPS):
            other = lax.rem(sub + step, subs)
            target = lax.rem(dom + offsets[g], doms)

            def signal():
                pl.semaphore_signal(barrier, inc=1, device_id=(target, other), device_id_type=pl.DeviceIdType.MESH)

            if g == 0:
                pl.when(step > 0)(signal)
            else:
                signal()
        return carry

    lax.fori_loop(0, subs, greet, 0)

    jflat[:, 0:2500] = jac_ref[...].astype(F32)
    jflat[:, 2500:2688] = jnp.zeros((24, 188), F32)
    for i in range(DOF):
        start = DOF * i
        tile = start // 128 * 128
        window = jflat[:, tile : tile + 256] if tile + 256 <= 2688 else jflat[:, 2432:2688]
        base = tile if tile + 256 <= 2688 else 2432
        jrows[i] = pltpu.roll(window, 256 - (start - base), 1)[:, 0:128]

    lane24 = lax.broadcasted_iota(jnp.int32, (24, 128), 1)
    row8 = lax.broadcasted_iota(jnp.int32, (8, 200), 0)

    def jacobi(vector):
        total = jnp.zeros((24, 128), F32)
        for i in range(DOF):
            entry = jnp.sum(jrows[i] * vector, axis=1, keepdims=True)
            total = jnp.where(lane24 == i, entry, total)
        return total

    sel_a, sel_s, sel_g, sel_b, sel_r, sel_f = (
        select_ref[first : first + rows].astype(BF16)
        for first, rows in ((0, 24), (24, 8), (32, 8), (40, 32), (72, 8), (80, 24))
    )

    pl.semaphore_wait(barrier, 31)

    def start_phase(phase, rows, sign):
        sbuf[phase] = rows

        def body(step, carry):
            other = lax.rem(sub + step, subs)
            for g in range(GROUPS):
                target = lax.rem(dom + (doms - offsets[g] if sign < 0 else offsets[g]), doms)

                def go():
                    pltpu.make_async_remote_copy(
                        src_ref=sbuf.at[phase, pl.ds(g, 1)],
                        dst_ref=rbuf.at[phase, pl.ds(g * subs + sub, 1)],
                        send_sem=send_sem.at[phase],
                        recv_sem=recv_sem.at[phase],
                        device_id=(target, other),
                        device_id_type=pl.DeviceIdType.MESH,
                    ).start()

                if g == 0:
                    pl.when(step > 0)(go)
                else:
                    go()
            return carry

        lax.fori_loop(0, subs, body, 0)

    def finish_phase(phase):
        whole = rbuf.at[phase, pl.ds(0, 31)]
        pltpu.make_async_copy(whole, whole, recv_sem.at[phase]).wait()
        return rbuf[phase]

    def start_chunk(chunk):
        width = 2560 // CHUNKS

        def body(step, carry):
            other = lax.rem(sub + step, subs)
            for g in range(GROUPS):
                target = lax.rem(dom + doms - offsets[g], doms)

                def go():
                    pltpu.make_async_remote_copy(
                        src_ref=sbig.at[chunk, g],
                        dst_ref=rbig.at[chunk, g * subs + sub],
                        send_sem=bsend_sem.at[chunk],
                        recv_sem=brecv_sem.at[chunk],
                        device_id=(target, other),
                        device_id_type=pl.DeviceIdType.MESH,
                    ).start()

                if g == 0:
                    pl.when(step > 0)(go)
                else:
                    go()
            return carry

        lax.fori_loop(0, subs, body, 0)

    def to_slots(wide):
        lane = lax.broadcasted_iota(jnp.int32, (8, 128), 1)
        pieces = []
        for side in range(4):
            turned = wide if side == 0 else pltpu.roll(wide, 256 - DOF * side, 1)
            pieces.append(jnp.where(lane < DOF, turned[:, 0:128], 0.0))
        return jnp.concatenate(pieces, axis=0)

    def to_elements(slots):
        zero = jnp.zeros((8, 128), F32)
        total = jnp.concatenate([slots[0:8], zero], axis=1)
        for side in range(1, 4):
            wide = jnp.concatenate([slots[8 * side : 8 * side + 8], zero], axis=1)
            total = total + pltpu.roll(wide, DOF * side, 1)
        return total

    def holder_rows(slots):
        stack = jnp.concatenate([slots, pltpu.roll(slots, 64, 1)], axis=0)
        return split_dot(sel_s[:, 0:64], stack)

    def owner_rows(traces):
        stack = jnp.concatenate([traces, pltpu.roll(traces, 64, 1)], axis=0)
        return split_dot(sel_g[:, 0:48], stack)

    def face_sum(slots, arrived):
        stack = jnp.concatenate([slots, arrived, pltpu.roll(arrived, 64, 1)], axis=0)
        total = split_dot(sel_a[:, 0:96], stack)
        return jnp.where(lane24 < DOF, total, 0.0)

    def slot_traces(traces, arrived):
        stack = jnp.concatenate([traces, arrived, pltpu.roll(arrived, 64, 1)], axis=0)
        total = split_dot(sel_b[:, 0:88], stack)
        lane = lax.broadcasted_iota(jnp.int32, (32, 128), 1)
        return jnp.where(lane < DOF, total, 0.0)

    def element_dots(elements, matrix_ref, rows):
        high = elements.astype(BF16).astype(F32)
        both = jnp.concatenate([high, elements - high], axis=0).astype(BF16)[:, 0:200]
        row = lax.broadcasted_iota(jnp.int32, (8, rows), 0)
        total = jnp.zeros((8, rows), F32)
        for e in range(8):
            out = lax.dot_general(both, matrix_ref[e], (((1,), (1,)), ((), ())), preferred_element_type=F32)
            total = jnp.where(row == e, out[0:8] + out[8:16], total)
        return total

    def wide(rows200):
        return jnp.concatenate([rows200, jnp.zeros((8, 56), F32)], axis=1)

    load_slots = to_slots(wide(fload_ref[...]))
    start_phase(0, holder_rows(load_slots), -1)

    blocks = blocks_ref[...]
    picked = jnp.dot(sel_r[:, 0:32], blocks, preferred_element_type=F32)
    width = 2560 // CHUNKS
    for chunk in range(CHUNKS):
        for g in range(GROUPS):
            sbig[chunk, g] = picked[2 * g : 2 * g + 2, chunk * width : (chunk + 1) * width]
    start_chunk(0)
    rhs = face_sum(load_slots, finish_phase(0))
    traces = jacobi(rhs)
    for sweep in range(SWEEPS):
        start_phase(2 * sweep + 1, owner_rows(traces), 1)
        start_chunk(2 * sweep + 1)
        elements = to_elements(slot_traces(traces, finish_phase(2 * sweep + 1)))
        slots = to_slots(wide(element_dots(elements, condensed_ref, 200)))
        start_phase(2 * sweep + 2, holder_rows(slots), -1)
        start_chunk(2 * sweep + 2)
        traces = traces + jacobi(rhs - face_sum(slots, finish_phase(2 * sweep + 2)))
    start_phase(5, owner_rows(traces), 1)
    trace_ref[...] = traces[:, 0:DOF]
    sum_faces = jnp.dot(sel_a[:, 0:32], blocks, preferred_element_type=F32)
    for chunk in range(CHUNKS):
        pltpu.make_async_copy(rbig.at[chunk, pl.ds(0, 31)], rbig.at[chunk, pl.ds(0, 31)], brecv_sem.at[chunk]).wait()
    far = []
    for g in range(GROUPS):
        index = g * subs + partner_ref[g]
        far.append(jnp.concatenate([rbig[chunk, index] for chunk in range(CHUNKS)], axis=1))
    far = jnp.concatenate(far, axis=0).astype(BF16)
    sum_faces = sum_faces + jnp.dot(
        sel_f[:, 0:8], far, preferred_element_type=F32
    )
    faces_ref[...] = sum_faces[:, 0:2500].astype(BF16)
    elements = to_elements(slot_traces(traces, finish_phase(5)))
    state_ref[...] = ((iload_ref[...] - element_dots(elements, imap_ref, 100)) * living_ref[...])
    for phase in range(6):
        whole = rbuf.at[phase, pl.ds(0, 31)]
        pltpu.make_async_copy(whole, whole, send_sem.at[phase]).wait()
    for chunk in range(CHUNKS):
        whole = rbig.at[chunk, pl.ds(0, 31)]
        pltpu.make_async_copy(whole, whole, bsend_sem.at[chunk]).wait()


def one_hots(slot_face, send_slot, recv_face, partner_sub, faces, subs):
    slot_of = slot_face.T.reshape(-1)
    sent = jnp.where(send_slot < 32, send_slot % 4 * 8 + send_slot // 4, -1)
    owned = jnp.where(recv_face < faces, recv_face, -1)
    face = jnp.arange(faces, dtype=jnp.int32)[:, None]
    slot = jnp.arange(32, dtype=jnp.int32)[:, None]
    each_sub = jnp.arange(subs, dtype=jnp.int32)[None, :]

    def from_sub(rows, partners):
        return jnp.where(partners[:, None] == each_sub, rows[:, None], -1).reshape(1, -1)

    def wide(table):
        table = table.astype(F32)
        return jnp.pad(table, ((0, 0), (0, 128 - table.shape[1])))

    holders, owners = partner_sub[:GROUPS], partner_sub[GROUPS:]
    table_a = jnp.concatenate(
        [slot_of[None, :], from_sub(owned[:, 0], holders), from_sub(owned[:, 1], holders)], axis=1
    )
    table_b = jnp.concatenate([from_sub(sent[:, 0], owners), from_sub(sent[:, 1], owners)], axis=1)
    slots_row, faces_row = slot.T, face.T
    pad4 = ((0, 8 - GROUPS), (0, 0))
    table_s = jnp.concatenate([sent[:, 0:1] == slots_row, sent[:, 1:2] == slots_row], axis=1)
    table_g = jnp.concatenate([owned[:, 0:1] == faces_row, owned[:, 1:2] == faces_row], axis=1)
    return jnp.concatenate(
        [
            wide(table_a == face),
            wide(jnp.pad(table_s, pad4)),
            wide(jnp.pad(table_g, pad4)),
            wide(jnp.concatenate([slot_of[:, None] == faces_row, table_b == slot], axis=1)),
            wide(sent.reshape(-1, 1) == slots_row),
            wide(owned.reshape(1, -1) == face),
        ],
        axis=0,
    )


def per_device(
    doms, subs,
    inv_interior, couple_if, couple_fi, face_face, load_interior, load_face, jacobi_inverse,
    slot_face, send_slot, recv_face, partner_sub, elem_count,
):
    elements = load_interior.shape[0]
    interior = load_interior.shape[1]
    face_width = load_face.shape[1]
    face_count = jacobi_inverse.shape[0]
    inverse_blocks = inv_interior.reshape(elements, interior, interior)
    couple_in = couple_if.reshape(elements, interior, face_width)
    couple_out = couple_fi.reshape(elements, face_width, interior)
    face_block = face_face.reshape(elements, face_width, face_width)
    living = (jnp.arange(elements, dtype=jnp.int32) < elem_count[0]).astype(F32)
    interior_map = jnp.einsum(
        "eij,ejk->eik", inverse_blocks, couple_in, preferred_element_type=F32
    ).astype(BF16)
    product = jnp.einsum("eij,ejk->eik", couple_out, interior_map, preferred_element_type=F32)
    condensed = ((face_block.astype(F32) - product) * living[:, None, None]).astype(BF16)
    interior_load = jnp.einsum(
        "eij,ej->ei", inverse_blocks.astype(F32), load_interior, precision=HIGH
    )
    face_load = (
        load_face - jnp.einsum("eij,ej->ei", couple_out.astype(F32), interior_load, precision=HIGH)
    ) * living[:, None]
    shaped = condensed.reshape(elements, 4, DOF, 4, DOF)
    blocks = jnp.concatenate(
        [shaped[:, side, :, side, :].reshape(elements, DOF * DOF) for side in range(4)], axis=0
    )
    blocks = jnp.pad(blocks, ((0, 0), (0, 60)))
    select = one_hots(slot_face, send_slot[0], recv_face[0], partner_sub[0], face_count, subs)
    vmem = pl.BlockSpec(memory_space=pltpu.VMEM)
    return pl.pallas_call(
        functools.partial(exchange_kernel, doms, subs),
        out_shape=(
            jax.ShapeDtypeStruct((face_count, DOF), F32),
            jax.ShapeDtypeStruct((elements, interior), F32),
            jax.ShapeDtypeStruct((face_count, DOF * DOF), BF16),
        ),
        in_specs=[vmem, pl.BlockSpec(memory_space=pltpu.SMEM)] + [vmem] * 7,
        out_specs=(vmem, vmem, vmem),
        scratch_shapes=[
            pltpu.VMEM((24, 2688), F32),
            pltpu.VMEM((DOF, 24, 128), F32),
            pltpu.VMEM((6, 8, 128), F32),
            pltpu.VMEM((6, 32, 128), F32),
            pltpu.VMEM((CHUNKS, GROUPS, 2, 2560 // CHUNKS), F32),
            pltpu.VMEM((CHUNKS, 32, 2, 2560 // CHUNKS), F32),
            pltpu.SemaphoreType.DMA((6,)),
            pltpu.SemaphoreType.DMA((6,)),
            pltpu.SemaphoreType.DMA((CHUNKS,)),
            pltpu.SemaphoreType.DMA((CHUNKS,)),
        ],
        compiler_params=pltpu.CompilerParams(collective_id=0, has_side_effects=True),
    )(select, partner_sub[0], condensed, interior_map, interior_load, face_load, jacobi_inverse, blocks, living[:, None])


def solution(mesh):
    rows = P(("dom", "sub"), None)
    placed = (rows,) * 8 + (P(("dom", "sub"), None, None),) * 2 + (rows, P(("dom", "sub")))
    return jax.shard_map(
        functools.partial(per_device, mesh.shape["dom"], mesh.shape["sub"]),
        mesh=mesh,
        in_specs=placed,
        out_specs=(rows, rows, rows),
        check_vma=False,
    )
```

```python
import functools

import jax
import jax.numpy as jnp
from jax import lax
from jax.experimental import pallas as pl
from jax.experimental.pallas import tpu as pltpu
from jax.sharding import PartitionSpec as P

HIGH = lax.Precision.HIGHEST
SWEEPS = 2
GROUPS = 4
DOF = 50
CHUNKS = 5
F32, BF16 = jnp.float32, jnp.bfloat16


def group_offset(group, doms):
    return [0, 1, doms // 2, doms - 1][group]


def split_dot(left, right):
    high = right.astype(BF16)
    low = (right - high.astype(F32)).astype(BF16)
    return jnp.dot(left, high, preferred_element_type=F32) + jnp.dot(
        left, low, preferred_element_type=F32
    )


def exchange_kernel(
    doms, subs,
    slot_ref, send_ref, recv_ref, partner_ref,
    condensed_ref, imap_ref, iload_ref, fload_ref, jac_ref, blocks_ref, living_ref,
    trace_ref, state_ref, faces_ref,
    jflat, jrows, sbuf, rbuf, sbig, rbig, send_sem, recv_sem, bsend_sem, brecv_sem,
):
    dom, sub = lax.axis_index("dom"), lax.axis_index("sub")
    offsets = [group_offset(g, doms) for g in range(GROUPS)]
    for phase in range(6):
        rbuf[phase] = jnp.zeros(rbuf.shape[1:], F32)
    barrier = pltpu.get_barrier_semaphore()

    def greet(step, carry):
        for g in range(GROUPS):
            other = lax.rem(sub + step, subs)
            target = lax.rem(dom + offsets[g], doms)

            def signal():
                pl.semaphore_signal(barrier, inc=1, device_id=(target, other), device_id_type=pl.DeviceIdType.MESH)

            if g == 0:
                pl.when(step > 0)(signal)
            else:
                signal()
        return carry

    lax.fori_loop(0, subs, greet, 0)

    jflat[:, 0:2500] = jac_ref[...].astype(F32)
    jflat[:, 2500:2688] = jnp.zeros((24, 188), F32)
    for i in range(DOF):
        start = DOF * i
        tile = start // 128 * 128
        window = jflat[:, tile : tile + 256] if tile + 256 <= 2688 else jflat[:, 2432:2688]
        base = tile if tile + 256 <= 2688 else 2432
        jrows[i] = pltpu.roll(window, 256 - (start - base), 1)[:, 0:128]

    lane24 = lax.broadcasted_iota(jnp.int32, (24, 128), 1)
    row8 = lax.broadcasted_iota(jnp.int32, (8, 200), 0)

    def jacobi(vector):
        total = jnp.zeros((24, 128), F32)
        for i in range(DOF):
            entry = jnp.sum(jrows[i] * vector, axis=1, keepdims=True)
            total = jnp.where(lane24 == i, entry, total)
        return total

    sel_a, sel_s, sel_g, sel_b, sel_r, sel_f = one_hots(slot_ref, send_ref, recv_ref, partner_ref, subs)

    pl.semaphore_wait(barrier, 31)

    def start_phase(phase, rows, sign):
        sbuf[phase] = rows

        def body(step, carry):
            other = lax.rem(sub + step, subs)
            for g in range(GROUPS):
                target = lax.rem(dom + (doms - offsets[g] if sign < 0 else offsets[g]), doms)

                def go():
                    pltpu.make_async_remote_copy(
                        src_ref=sbuf.at[phase, pl.ds(g, 1)],
                        dst_ref=rbuf.at[phase, pl.ds(g * subs + sub, 1)],
                        send_sem=send_sem.at[phase],
                        recv_sem=recv_sem.at[phase],
                        device_id=(target, other),
                        device_id_type=pl.DeviceIdType.MESH,
                    ).start()

                if g == 0:
                    pl.when(step > 0)(go)
                else:
                    go()
            return carry

        lax.fori_loop(0, subs, body, 0)

    def finish_phase(phase):
        whole = rbuf.at[phase, pl.ds(0, 31)]
        pltpu.make_async_copy(whole, whole, recv_sem.at[phase]).wait()
        return rbuf[phase]

    def start_chunk(chunk):
        width = 2560 // CHUNKS

        def body(step, carry):
            other = lax.rem(sub + step, subs)
            for g in range(GROUPS):
                target = lax.rem(dom + doms - offsets[g], doms)

                def go():
                    pltpu.make_async_remote_copy(
                        src_ref=sbig.at[chunk, g],
                        dst_ref=rbig.at[chunk, g * subs + sub],
                        send_sem=bsend_sem.at[chunk],
                        recv_sem=brecv_sem.at[chunk],
                        device_id=(target, other),
                        device_id_type=pl.DeviceIdType.MESH,
                    ).start()

                if g == 0:
                    pl.when(step > 0)(go)
                else:
                    go()
            return carry

        lax.fori_loop(0, subs, body, 0)

    def to_slots(wide):
        lane = lax.broadcasted_iota(jnp.int32, (8, 128), 1)
        pieces = []
        for side in range(4):
            turned = wide if side == 0 else pltpu.roll(wide, 256 - DOF * side, 1)
            pieces.append(jnp.where(lane < DOF, turned[:, 0:128], 0.0))
        return jnp.concatenate(pieces, axis=0)

    def to_elements(slots):
        zero = jnp.zeros((8, 128), F32)
        total = jnp.concatenate([slots[0:8], zero], axis=1)
        for side in range(1, 4):
            wide = jnp.concatenate([slots[8 * side : 8 * side + 8], zero], axis=1)
            total = total + pltpu.roll(wide, DOF * side, 1)
        return total

    def holder_rows(slots):
        stack = jnp.concatenate([slots, pltpu.roll(slots, 64, 1)], axis=0)
        return split_dot(sel_s[:, 0:64], stack)

    def owner_rows(traces):
        stack = jnp.concatenate([traces, pltpu.roll(traces, 64, 1)], axis=0)
        return split_dot(sel_g[:, 0:48], stack)

    def face_sum(slots, arrived):
        stack = jnp.concatenate([slots, arrived, pltpu.roll(arrived, 64, 1)], axis=0)
        total = split_dot(sel_a[:, 0:96], stack)
        return jnp.where(lane24 < DOF, total, 0.0)

    def slot_traces(traces, arrived):
        stack = jnp.concatenate([traces, arrived, pltpu.roll(arrived, 64, 1)], axis=0)
        total = split_dot(sel_b[:, 0:88], stack)
        lane = lax.broadcasted_iota(jnp.int32, (32, 128), 1)
        return jnp.where(lane < DOF, total, 0.0)

    def element_dots(elements, matrix_ref, rows):
        high = elements.astype(BF16).astype(F32)
        both = jnp.concatenate([high, elements - high], axis=0).astype(BF16)[:, 0:200]
        row = lax.broadcasted_iota(jnp.int32, (8, rows), 0)
        total = jnp.zeros((8, rows), F32)
        for e in range(8):
            out = lax.dot_general(both, matrix_ref[e], (((1,), (1,)), ((), ())), preferred_element_type=F32)
            total = jnp.where(row == e, out[0:8] + out[8:16], total)
        return total

    def wide(rows200):
        return jnp.concatenate([rows200, jnp.zeros((8, 56), F32)], axis=1)

    load_slots = to_slots(wide(fload_ref[...]))
    start_phase(0, holder_rows(load_slots), -1)

    blocks = blocks_ref[...]
    picked = jnp.dot(sel_r[:, 0:32], blocks, preferred_element_type=F32)
    width = 2560 // CHUNKS
    for chunk in range(CHUNKS):
        for g in range(GROUPS):
            sbig[chunk, g] = picked[2 * g : 2 * g + 2, chunk * width : (chunk + 1) * width]
    start_chunk(0)
    rhs = face_sum(load_slots, finish_phase(0))
    traces = jacobi(rhs)
    for sweep in range(SWEEPS):
        start_phase(2 * sweep + 1, owner_rows(traces), 1)
        start_chunk(2 * sweep + 1)
        elements = to_elements(slot_traces(traces, finish_phase(2 * sweep + 1)))
        slots = to_slots(wide(element_dots(elements, condensed_ref, 200)))
        start_phase(2 * sweep + 2, holder_rows(slots), -1)
        start_chunk(2 * sweep + 2)
        traces = traces + jacobi(rhs - face_sum(slots, finish_phase(2 * sweep + 2)))
    start_phase(5, owner_rows(traces), 1)
    trace_ref[...] = traces[:, 0:DOF]
    sum_faces = jnp.dot(sel_a[:, 0:32], blocks, preferred_element_type=F32)
    for chunk in range(CHUNKS):
        pltpu.make_async_copy(rbig.at[chunk, pl.ds(0, 31)], rbig.at[chunk, pl.ds(0, 31)], brecv_sem.at[chunk]).wait()
    far = []
    for g in range(GROUPS):
        index = g * subs + partner_ref[0, g]
        far.append(jnp.concatenate([rbig[chunk, index] for chunk in range(CHUNKS)], axis=1))
    far = jnp.concatenate(far, axis=0).astype(BF16)
    sum_faces = sum_faces + jnp.dot(
        sel_f[:, 0:8], far, preferred_element_type=F32
    )
    faces_ref[...] = sum_faces[:, 0:2500].astype(BF16)
    elements = to_elements(slot_traces(traces, finish_phase(5)))
    state_ref[...] = ((iload_ref[...] - element_dots(elements, imap_ref, 100)) * living_ref[...])
    for phase in range(6):
        whole = rbuf.at[phase, pl.ds(0, 31)]
        pltpu.make_async_copy(whole, whole, send_sem.at[phase]).wait()
    for chunk in range(CHUNKS):
        whole = rbig.at[chunk, pl.ds(0, 31)]
        pltpu.make_async_copy(whole, whole, bsend_sem.at[chunk]).wait()


def one_hots(slot_ref, send_ref, recv_ref, partner_ref, subs):
    lane = lax.broadcasted_iota(jnp.int32, (8, 128), 1)
    row = lax.broadcasted_iota(jnp.int32, (8, 128), 0)
    row24 = lax.broadcasted_iota(jnp.int32, (24, 128), 0)
    row32 = lax.broadcasted_iota(jnp.int32, (32, 128), 0)
    nothing = jnp.full((8, 128), -1, jnp.int32)
    no = jnp.zeros((8, 128), F32)
    table_a, table_b, table_f, hot_s, hot_g, hot_r, local_b = nothing, nothing, nothing, no, no, no, []
    for side in range(4):
        column = nothing
        for e in range(8):
            face = slot_ref[side, e]
            face = jnp.where(face < 24, face, -1)
            table_a = jnp.where(lane == 8 * side + e, face, table_a)
            column = jnp.where(row == e, face, column)
        local_b.append((lane == column).astype(F32))
    for g in range(GROUPS):
        holder, owner = partner_ref[0, g], partner_ref[0, GROUPS + g]
        for r in range(2):
            face, slot = recv_ref[0, r, g], send_ref[0, r, g]
            face = jnp.where(face < 24, face, -1000)
            slot = jnp.where(slot < 32, (slot & 3) * 8 + (slot >> 2), -1000)
            table_a = jnp.where(lane == 32 + 32 * r + subs * g + holder, face, table_a)
            table_b = jnp.where(lane == 24 + 32 * r + subs * g + owner, slot, table_b)
            table_f = jnp.where(lane == 2 * g + r, face, table_f)
            hot_s = jnp.where((row == g) & (lane == 32 * r + slot), 1.0, hot_s)
            hot_g = jnp.where((row == g) & (lane == 24 * r + face), 1.0, hot_g)
            hot_r = jnp.where((row == 2 * g + r) & (lane == slot), 1.0, hot_r)

    def equal(rows, table):
        return (rows == jnp.concatenate([table] * (rows.shape[0] // 8), axis=0)).astype(F32)

    hot_b = equal(row32, table_b) + jnp.concatenate(local_b, axis=0)
    hots = (equal(row24, table_a), hot_s, hot_g, hot_b, hot_r, equal(row24, table_f))
    return tuple(hot.astype(BF16) for hot in hots)


def squeeze_kernel(*refs):
    half = len(refs) // 2
    for source, target in zip(refs[:half], refs[half:]):
        rows = target.shape[0]
        for first in range(0, rows, 16):
            count = min(16, rows - first)
            line = source[0:1, 128 * first : 128 * (first + count)].astype(F32)
            target[first : first + count, :] = line.reshape(count, 128).astype(BF16)


def squeezed(*arrays):
    vmem = pl.BlockSpec(memory_space=pltpu.VMEM)
    return pl.pallas_call(
        squeeze_kernel,
        out_shape=[jax.ShapeDtypeStruct((array.shape[1] // 128, 128), BF16) for array in arrays],
        in_specs=[vmem] * len(arrays),
        out_specs=[vmem] * len(arrays),
    )(*arrays)


def per_device(
    doms, subs,
    inv_interior, couple_if, couple_fi, face_face, load_interior, load_face, jacobi_inverse,
    slot_face, send_slot, recv_face, partner_sub, elem_count,
):
    elements = load_interior.shape[0]
    interior = load_interior.shape[1]
    face_width = load_face.shape[1]
    face_count = jacobi_inverse.shape[0]
    inv_interior, couple_if, couple_fi, face_face = squeezed(inv_interior, couple_if, couple_fi, face_face)
    inverse_blocks = inv_interior.reshape(elements, interior, interior)
    couple_in = couple_if.reshape(elements, interior, face_width)
    couple_out = couple_fi.reshape(elements, face_width, interior)
    face_block = face_face.reshape(elements, face_width, face_width)
    living = (jnp.arange(elements, dtype=jnp.int32) < elem_count[0]).astype(F32)
    interior_map = jnp.einsum(
        "eij,ejk->eik", inverse_blocks, couple_in, preferred_element_type=F32
    ).astype(BF16)
    product = jnp.einsum("eij,ejk->eik", couple_out, interior_map, preferred_element_type=F32)
    condensed = ((face_block.astype(F32) - product) * living[:, None, None]).astype(BF16)
    interior_load = jnp.einsum(
        "eij,ej->ei", inverse_blocks.astype(F32), load_interior, precision=HIGH
    )
    face_load = (
        load_face - jnp.einsum("eij,ej->ei", couple_out.astype(F32), interior_load, precision=HIGH)
    ) * living[:, None]
    shaped = condensed.reshape(elements, 4, DOF, 4, DOF)
    blocks = jnp.concatenate(
        [shaped[:, side, :, side, :].reshape(elements, DOF * DOF) for side in range(4)], axis=0
    )
    blocks = jnp.pad(blocks, ((0, 0), (0, 60)))
    vmem = pl.BlockSpec(memory_space=pltpu.VMEM)
    return pl.pallas_call(
        functools.partial(exchange_kernel, doms, subs),
        out_shape=(
            jax.ShapeDtypeStruct((face_count, DOF), F32),
            jax.ShapeDtypeStruct((elements, interior), F32),
            jax.ShapeDtypeStruct((face_count, DOF * DOF), BF16),
        ),
        in_specs=[pl.BlockSpec(memory_space=pltpu.SMEM)] * 4 + [vmem] * 7,
        out_specs=(vmem, vmem, vmem),
        scratch_shapes=[
            pltpu.VMEM((24, 2688), F32),
            pltpu.VMEM((DOF, 24, 128), F32),
            pltpu.VMEM((6, 8, 128), F32),
            pltpu.VMEM((6, 32, 128), F32),
            pltpu.VMEM((CHUNKS, GROUPS, 2, 2560 // CHUNKS), F32),
            pltpu.VMEM((CHUNKS, 32, 2, 2560 // CHUNKS), F32),
            pltpu.SemaphoreType.DMA((6,)),
            pltpu.SemaphoreType.DMA((6,)),
            pltpu.SemaphoreType.DMA((CHUNKS,)),
            pltpu.SemaphoreType.DMA((CHUNKS,)),
        ],
        compiler_params=pltpu.CompilerParams(collective_id=0, has_side_effects=True),
    )(slot_face.T, send_slot.transpose(0, 2, 1), recv_face.transpose(0, 2, 1), partner_sub, condensed, interior_map, interior_load, face_load, jacobi_inverse, blocks, living[:, None])


def solution(mesh):
    rows = P(("dom", "sub"), None)
    placed = (rows,) * 8 + (P(("dom", "sub"), None, None),) * 2 + (rows, P(("dom", "sub")))
    return jax.shard_map(
        functools.partial(per_device, mesh.shape["dom"], mesh.shape["sub"]),
        mesh=mesh,
        in_specs=placed,
        out_specs=(rows, rows, rows),
        check_vma=False,
    )
```

```python
import functools

import jax
import jax.numpy as jnp
from jax import lax
from jax.experimental import pallas as pl
from jax.experimental.pallas import tpu as pltpu
from jax.sharding import PartitionSpec as P

HIGH = lax.Precision.HIGHEST
SWEEPS = 2
GROUPS = 4
DOF = 50
CHUNKS = 5
F32, BF16 = jnp.float32, jnp.bfloat16


def group_offset(group, doms):
    return [0, 1, doms // 2, doms - 1][group]


def split_dot(left, right):
    high = right.astype(BF16)
    low = (right - high.astype(F32)).astype(BF16)
    return jnp.dot(left, high, preferred_element_type=F32) + jnp.dot(
        left, low, preferred_element_type=F32
    )


def exchange_kernel(
    doms, subs,
    slot_ref, send_ref, recv_ref, partner_ref, count_ref,
    inv_hbm, cif_hbm, cfi_hbm, ff_hbm, load_ref, fload_ref, jac_ref,
    trace_ref, state_ref, faces_ref,
    jflat, jrows, sbuf, rbuf, sbig, rbig, send_sem, recv_sem, bsend_sem, brecv_sem,
    inv_ref, cif_ref, cfi_ref, ff_ref, in_sem, condensed_ref, imap_ref, iload_ref, face_load_ref, blocks_ref,
    *spaces,
):
    dom, sub = lax.axis_index("dom"), lax.axis_index("sub")
    loads = [
        pltpu.make_async_copy(source, target, in_sem.at[k])
        for k, (source, target) in enumerate(
            ((inv_hbm, inv_ref), (cfi_hbm, cfi_ref), (cif_hbm, cif_ref), (ff_hbm, ff_ref))
        )
    ]
    for load in loads:
        load.start()
    offsets = [group_offset(g, doms) for g in range(GROUPS)]
    for phase in range(6):
        rbuf[phase] = jnp.zeros(rbuf.shape[1:], F32)
    barrier = pltpu.get_barrier_semaphore()

    def greet(step, carry):
        for g in range(GROUPS):
            other = lax.rem(sub + step, subs)
            target = lax.rem(dom + offsets[g], doms)

            def signal():
                pl.semaphore_signal(barrier, inc=1, device_id=(target, other), device_id_type=pl.DeviceIdType.MESH)

            if g == 0:
                pl.when(step > 0)(signal)
            else:
                signal()
        return carry

    lax.fori_loop(0, subs, greet, 0)

    condense_body(
        loads, inv_ref, cif_ref, cfi_ref, ff_ref, load_ref, fload_ref, count_ref,
        condensed_ref, imap_ref, iload_ref, face_load_ref, blocks_ref, *spaces,
    )

    jflat[:, 0:2500] = jac_ref[...].astype(F32)
    jflat[:, 2500:2688] = jnp.zeros((24, 188), F32)
    for i in range(DOF):
        start = DOF * i
        tile = start // 128 * 128
        window = jflat[:, tile : tile + 256] if tile + 256 <= 2688 else jflat[:, 2432:2688]
        base = tile if tile + 256 <= 2688 else 2432
        jrows[i] = pltpu.roll(window, 256 - (start - base), 1)[:, 0:128]

    lane24 = lax.broadcasted_iota(jnp.int32, (24, 128), 1)

    def jacobi(vector):
        total = jnp.zeros((24, 128), F32)
        for i in range(DOF):
            entry = jnp.sum(jrows[i] * vector, axis=1, keepdims=True)
            total = jnp.where(lane24 == i, entry, total)
        return total

    sel_a, sel_s, sel_g, sel_b, sel_r, sel_f = one_hots(slot_ref, send_ref, recv_ref, partner_ref, subs)

    pl.semaphore_wait(barrier, 31)

    def start_phase(phase, rows, sign):
        sbuf[phase] = rows

        def body(step, carry):
            other = lax.rem(sub + step, subs)
            for g in range(GROUPS):
                target = lax.rem(dom + (doms - offsets[g] if sign < 0 else offsets[g]), doms)

                def go():
                    pltpu.make_async_remote_copy(
                        src_ref=sbuf.at[phase, pl.ds(g, 1)],
                        dst_ref=rbuf.at[phase, pl.ds(g * subs + sub, 1)],
                        send_sem=send_sem.at[phase],
                        recv_sem=recv_sem.at[phase],
                        device_id=(target, other),
                        device_id_type=pl.DeviceIdType.MESH,
                    ).start()

                if g == 0:
                    pl.when(step > 0)(go)
                else:
                    go()
            return carry

        lax.fori_loop(0, subs, body, 0)

    def finish_phase(phase):
        whole = rbuf.at[phase, pl.ds(0, 31)]
        pltpu.make_async_copy(whole, whole, recv_sem.at[phase]).wait()
        return rbuf[phase]

    def start_chunk(chunk):
        width = 2560 // CHUNKS

        def body(step, carry):
            other = lax.rem(sub + step, subs)
            for g in range(GROUPS):
                target = lax.rem(dom + doms - offsets[g], doms)

                def go():
                    pltpu.make_async_remote_copy(
                        src_ref=sbig.at[chunk, g],
                        dst_ref=rbig.at[chunk, g * subs + sub],
                        send_sem=bsend_sem.at[chunk],
                        recv_sem=brecv_sem.at[chunk],
                        device_id=(target, other),
                        device_id_type=pl.DeviceIdType.MESH,
                    ).start()

                if g == 0:
                    pl.when(step > 0)(go)
                else:
                    go()
            return carry

        lax.fori_loop(0, subs, body, 0)

    def to_slots(wide):
        lane = lax.broadcasted_iota(jnp.int32, (8, 128), 1)
        pieces = []
        for side in range(4):
            turned = wide if side == 0 else pltpu.roll(wide, 256 - DOF * side, 1)
            pieces.append(jnp.where(lane < DOF, turned[:, 0:128], 0.0))
        return jnp.concatenate(pieces, axis=0)

    def to_elements(slots):
        zero = jnp.zeros((8, 128), F32)
        total = jnp.concatenate([slots[0:8], zero], axis=1)
        for side in range(1, 4):
            wide = jnp.concatenate([slots[8 * side : 8 * side + 8], zero], axis=1)
            total = total + pltpu.roll(wide, DOF * side, 1)
        return total

    def holder_rows(slots):
        stack = jnp.concatenate([slots, pltpu.roll(slots, 64, 1)], axis=0)
        return split_dot(sel_s[:, 0:64], stack)

    def owner_rows(traces):
        stack = jnp.concatenate([traces, pltpu.roll(traces, 64, 1)], axis=0)
        return split_dot(sel_g[:, 0:48], stack)

    def face_sum(slots, arrived):
        stack = jnp.concatenate([slots, arrived, pltpu.roll(arrived, 64, 1)], axis=0)
        total = split_dot(sel_a[:, 0:96], stack)
        return jnp.where(lane24 < DOF, total, 0.0)

    def slot_traces(traces, arrived):
        stack = jnp.concatenate([traces, arrived, pltpu.roll(arrived, 64, 1)], axis=0)
        total = split_dot(sel_b[:, 0:88], stack)
        lane = lax.broadcasted_iota(jnp.int32, (32, 128), 1)
        return jnp.where(lane < DOF, total, 0.0)

    def element_dots(elements, matrix_ref, rows):
        high = elements.astype(BF16).astype(F32)
        both = jnp.concatenate([high, elements - high], axis=0).astype(BF16)[:, 0:200]
        row = lax.broadcasted_iota(jnp.int32, (8, rows), 0)
        total = jnp.zeros((8, rows), F32)
        for e in range(8):
            out = lax.dot_general(both, matrix_ref[e], (((1,), (1,)), ((), ())), preferred_element_type=F32)
            total = jnp.where(row == e, out[0:8] + out[8:16], total)
        return total

    def wide(rows200):
        return jnp.concatenate([rows200, jnp.zeros((8, 56), F32)], axis=1)

    load_slots = to_slots(wide(face_load_ref[...]))
    start_phase(0, holder_rows(load_slots), -1)

    blocks = blocks_ref[...]
    picked = jnp.dot(sel_r[:, 0:32], blocks, preferred_element_type=F32)
    width = 2560 // CHUNKS
    for chunk in range(CHUNKS):
        for g in range(GROUPS):
            sbig[chunk, g] = picked[2 * g : 2 * g + 2, chunk * width : (chunk + 1) * width]
    start_chunk(0)
    rhs = face_sum(load_slots, finish_phase(0))
    traces = jacobi(rhs)
    for sweep in range(SWEEPS):
        start_phase(2 * sweep + 1, owner_rows(traces), 1)
        start_chunk(2 * sweep + 1)
        elements = to_elements(slot_traces(traces, finish_phase(2 * sweep + 1)))
        slots = to_slots(wide(element_dots(elements, condensed_ref, 200)))
        start_phase(2 * sweep + 2, holder_rows(slots), -1)
        start_chunk(2 * sweep + 2)
        traces = traces + jacobi(rhs - face_sum(slots, finish_phase(2 * sweep + 2)))
    start_phase(5, owner_rows(traces), 1)
    trace_ref[...] = traces
    sum_faces = jnp.dot(sel_a[:, 0:32], blocks, preferred_element_type=F32)
    for chunk in range(CHUNKS):
        pltpu.make_async_copy(rbig.at[chunk, pl.ds(0, 31)], rbig.at[chunk, pl.ds(0, 31)], brecv_sem.at[chunk]).wait()
    far = []
    for g in range(GROUPS):
        index = g * subs + partner_ref[0, g]
        far.append(jnp.concatenate([rbig[chunk, index] for chunk in range(CHUNKS)], axis=1))
    far = jnp.concatenate(far, axis=0).astype(BF16)
    sum_faces = sum_faces + jnp.dot(
        sel_f[:, 0:8], far, preferred_element_type=F32
    )
    faces_ref[...] = sum_faces
    elements = to_elements(slot_traces(traces, finish_phase(5)))
    row100 = lax.broadcasted_iota(jnp.int32, (8, 100), 0)
    state = iload_ref[...] - element_dots(elements, imap_ref, 100)
    state = jnp.where(row100 < count_ref[0], state, 0.0)
    state_ref[...] = jnp.concatenate([state, jnp.zeros((8, 28), F32)], axis=1)
    for phase in range(6):
        whole = rbuf.at[phase, pl.ds(0, 31)]
        pltpu.make_async_copy(whole, whole, send_sem.at[phase]).wait()
    for chunk in range(CHUNKS):
        whole = rbig.at[chunk, pl.ds(0, 31)]
        pltpu.make_async_copy(whole, whole, bsend_sem.at[chunk]).wait()


def one_hots(slot_ref, send_ref, recv_ref, partner_ref, subs):
    lane = lax.broadcasted_iota(jnp.int32, (8, 128), 1)
    row = lax.broadcasted_iota(jnp.int32, (8, 128), 0)
    row24 = lax.broadcasted_iota(jnp.int32, (24, 128), 0)
    row32 = lax.broadcasted_iota(jnp.int32, (32, 128), 0)
    nothing = jnp.full((8, 128), -1, jnp.int32)
    no = jnp.zeros((8, 128), F32)
    table_a, table_b, table_f, hot_s, hot_g, hot_r, local_b = nothing, nothing, nothing, no, no, no, []
    for side in range(4):
        column = nothing
        for e in range(8):
            face = slot_ref[side, e]
            face = jnp.where(face < 24, face, -1)
            table_a = jnp.where(lane == 8 * side + e, face, table_a)
            column = jnp.where(row == e, face, column)
        local_b.append((lane == column).astype(F32))
    for g in range(GROUPS):
        holder, owner = partner_ref[0, g], partner_ref[0, GROUPS + g]
        for r in range(2):
            face, slot = recv_ref[0, r, g], send_ref[0, r, g]
            face = jnp.where(face < 24, face, -1000)
            slot = jnp.where(slot < 32, (slot & 3) * 8 + (slot >> 2), -1000)
            table_a = jnp.where(lane == 32 + 32 * r + subs * g + holder, face, table_a)
            table_b = jnp.where(lane == 24 + 32 * r + subs * g + owner, slot, table_b)
            table_f = jnp.where(lane == 2 * g + r, face, table_f)
            hot_s = jnp.where((row == g) & (lane == 32 * r + slot), 1.0, hot_s)
            hot_g = jnp.where((row == g) & (lane == 24 * r + face), 1.0, hot_g)
            hot_r = jnp.where((row == 2 * g + r) & (lane == slot), 1.0, hot_r)

    def equal(rows, table):
        return (rows == jnp.concatenate([table] * (rows.shape[0] // 8), axis=0)).astype(F32)

    hot_b = equal(row32, table_b) + jnp.concatenate(local_b, axis=0)
    hots = (equal(row24, table_a), hot_s, hot_g, hot_b, hot_r, equal(row24, table_f))
    return tuple(hot.astype(BF16) for hot in hots)


def squeeze(source, flat):
    rows = source.shape[1] // 128
    for first in range(0, rows, 16):
        count = min(16, rows - first)
        line = source[0:1, 128 * first : 128 * (first + count)].astype(F32)
        flat[first : first + count, :] = line.reshape(count, 128)


def spread_rows(flat, mid, width, count, pitch):
    lane = lax.broadcasted_iota(jnp.int32, (count, 128), 1)
    for i in range(3200 // width):
        first, off = divmod(width * i, 128)
        last = (off + width - 1) // 128
        turned = []
        for tile in range(last + 1):
            value = flat[pl.ds(first + tile, count, stride=25), :]
            turned.append(pltpu.roll(value, 128 - off, 1) if off else value)
        for tile in range((width + 127) // 128):
            value = turned[tile]
            if off and tile < last:
                value = jnp.where(lane < 128 - off, value, turned[tile + 1])
            mid[tile, pl.ds(i * pitch, count), :] = value


def matrix_rows(mid, tile, first, rows, period, pitch):
    pieces = []
    for m in range(first, first + rows, 8):
        size = min(8, first + rows - m)
        p, i = divmod(m, period)
        for start, stop in ((i, min(i + size, period)), (period, i + size)):
            if stop > start:
                at = start % period * pitch + p + start // period
                pieces.append(mid[tile, pl.ds(at, stop - start, stride=pitch), :])
    return jnp.concatenate(pieces, axis=0)


def matrix(mid, e, rows, width, pitch):
    period = 3200 // width
    tiles = [matrix_rows(mid, tile, e * rows, rows, period, pitch) for tile in range((width + 127) // 128)]
    whole = tiles[0] if len(tiles) == 1 else jnp.concatenate(tiles, axis=1)
    return whole[:, 0:width]


def two_terms(rows):
    high = rows.astype(BF16).astype(F32)
    return jnp.concatenate([high, rows - high], axis=0).astype(BF16)


def times_transposed(both, right):
    out = lax.dot_general(both, right, (((1,), (1,)), ((), ())), preferred_element_type=F32)
    return out[0:8] + out[8:16]


def condense_body(
    loads, inv_ref, cif_ref, cfi_ref, ff_ref, load_ref, fload_ref, count_ref,
    condensed_ref, imap_ref, iload_ref, face_load_ref, blocks_ref,
    flat_inv, flat_cif, flat_cfi, flat_ff, mid_inv, mid_cif, mid_cfi, mid_ff, wide,
):
    loads[0].wait()
    squeeze(inv_ref, flat_inv)
    loads[1].wait()
    squeeze(cfi_ref, flat_cfi)
    spread_rows(flat_inv, mid_inv, 100, 32, 33)
    spread_rows(flat_cfi, mid_cfi, 100, 56, 57)
    loads[2].wait()
    squeeze(cif_ref, flat_cif)
    loads[3].wait()
    squeeze(ff_ref, flat_ff)
    spread_rows(flat_cif, mid_cif, 200, 56, 57)
    spread_rows(flat_ff, mid_ff, 200, 104, 105)
    count = count_ref[0]
    row100 = lax.broadcasted_iota(jnp.int32, (8, 100), 0)
    row200 = lax.broadcasted_iota(jnp.int32, (8, 200), 0)
    both = two_terms(load_ref[...])
    iload = jnp.zeros((8, 100), F32)
    for e in range(8):
        inverse = matrix(mid_inv, e, 100, 100, 33).astype(BF16)
        iload = jnp.where(row100 == e, times_transposed(both, inverse), iload)
        inner = matrix(mid_cif, e, 100, 200, 57).astype(BF16)
        imap_ref[e] = jnp.dot(inverse, inner, preferred_element_type=F32).astype(BF16)
    iload_ref[...] = iload
    both = two_terms(iload)
    outer_load = jnp.zeros((8, 200), F32)
    for e in range(8):
        outer = matrix(mid_cfi, e, 200, 100, 57).astype(BF16)
        outer_load = jnp.where(row200 == e, times_transposed(both, outer), outer_load)
        product = jnp.dot(outer, imap_ref[e], preferred_element_type=F32)
        alive = jnp.where(e < count, 1.0, 0.0)
        block = ((matrix(mid_ff, e, 200, 200, 105) - product) * alive).astype(BF16)
        condensed_ref[e] = block
        block = block.astype(F32)
        wide[0, 200 * e : 200 * e + 200, :] = block[:, 0:128]
        wide[1, 200 * e : 200 * e + 200, :] = jnp.concatenate([block[:, 128:200], jnp.zeros((200, 56), F32)], axis=1)
    face_load_ref[...] = jnp.where(row200 < count, fload_ref[...] - outer_load, 0.0)

    lane = lax.broadcasted_iota(jnp.int32, (8, 128), 1)
    for side in range(4):
        start = DOF * side
        tiles = [jnp.zeros((8, 128), F32) for _ in range(20)]
        for i in range(DOF):
            at = pl.ds(start + i, 8, stride=200)
            if side == 2:
                value = jnp.where(lane < 64, wide[1, at, :], wide[0, at, :])
            else:
                value = wide[start // 128, at, :]
            tile, off = divmod(DOF * i, 128)
            shift = (off - start) % 128
            value = pltpu.roll(value, shift, 1) if shift else value
            tiles[tile] = jnp.where((lane >= off) & (lane < off + DOF), value, tiles[tile])
            if off + DOF > 128:
                tiles[tile + 1] = jnp.where(lane < off + DOF - 128, value, tiles[tile + 1])
        blocks_ref[8 * side : 8 * side + 8, :] = jnp.concatenate(tiles, axis=1).astype(BF16)


def finish_kernel(trace_ref, state_ref, faces_ref, trace_out, state_out, faces_out):
    trace_out[...] = trace_ref[:, 0:DOF]
    state_out[...] = state_ref[:, 0:100]
    faces_out[...] = faces_ref[:, 0 : DOF * DOF].astype(BF16)


def per_device(
    doms, subs,
    inv_interior, couple_if, couple_fi, face_face, load_interior, load_face, jacobi_inverse,
    slot_face, send_slot, recv_face, partner_sub, elem_count,
):
    vmem = pl.BlockSpec(memory_space=pltpu.VMEM)
    smem = pl.BlockSpec(memory_space=pltpu.SMEM)
    part = 2560 // CHUNKS
    results = pl.pallas_call(
        functools.partial(exchange_kernel, doms, subs),
        out_shape=(
            jax.ShapeDtypeStruct((24, 128), F32),
            jax.ShapeDtypeStruct((8, 128), F32),
            jax.ShapeDtypeStruct((24, 2560), F32),
        ),
        in_specs=[smem] * 5 + [pl.BlockSpec(memory_space=pl.ANY)] * 4 + [vmem] * 3,
        out_specs=(vmem, vmem, vmem),
        scratch_shapes=[
            pltpu.VMEM((24, 2688), F32),
            pltpu.VMEM((DOF, 24, 128), F32),
            pltpu.VMEM((6, 8, 128), F32),
            pltpu.VMEM((6, 32, 128), F32),
            pltpu.VMEM((CHUNKS, GROUPS, 2, part), F32),
            pltpu.VMEM((CHUNKS, 32, 2, part), F32),
            pltpu.SemaphoreType.DMA((6,)),
            pltpu.SemaphoreType.DMA((6,)),
            pltpu.SemaphoreType.DMA((CHUNKS,)),
            pltpu.SemaphoreType.DMA((CHUNKS,)),
            pltpu.VMEM(inv_interior.shape, BF16),
            pltpu.VMEM(couple_if.shape, BF16),
            pltpu.VMEM(couple_fi.shape, BF16),
            pltpu.VMEM(face_face.shape, BF16),
            pltpu.SemaphoreType.DMA((4,)),
            pltpu.VMEM((8, 200, 200), BF16),
            pltpu.VMEM((8, 100, 200), BF16),
            pltpu.VMEM((8, 100), F32),
            pltpu.VMEM((8, 200), F32),
            pltpu.VMEM((32, 2560), BF16),
            pltpu.VMEM((808, 128), F32),
            pltpu.VMEM((1408, 128), F32),
            pltpu.VMEM((1408, 128), F32),
            pltpu.VMEM((2608, 128), F32),
            pltpu.VMEM((1, 1064, 128), F32),
            pltpu.VMEM((2, 920, 128), F32),
            pltpu.VMEM((1, 1832, 128), F32),
            pltpu.VMEM((2, 1688, 128), F32),
            pltpu.VMEM((2, 1600, 128), F32),
        ],
        compiler_params=pltpu.CompilerParams(collective_id=0, has_side_effects=True),
    )(
        slot_face.T, send_slot.transpose(0, 2, 1), recv_face.transpose(0, 2, 1), partner_sub, elem_count,
        inv_interior, couple_if, couple_fi, face_face, load_interior, load_face, jacobi_inverse,
    )
    return pl.pallas_call(
        finish_kernel,
        out_shape=(
            jax.ShapeDtypeStruct((24, DOF), F32),
            jax.ShapeDtypeStruct((8, 100), F32),
            jax.ShapeDtypeStruct((24, DOF * DOF), BF16),
        ),
        in_specs=[vmem] * 3,
        out_specs=(vmem, vmem, vmem),
    )(*results)


def solution(mesh):
    rows = P(("dom", "sub"), None)
    placed = (rows,) * 8 + (P(("dom", "sub"), None, None),) * 2 + (rows, P(("dom", "sub")))
    return jax.shard_map(
        functools.partial(per_device, mesh.shape["dom"], mesh.shape["sub"]),
        mesh=mesh,
        in_specs=placed,
        out_specs=(rows, rows, rows),
        check_vma=False,
    )
```

```python
import functools

import jax
import jax.numpy as jnp
from jax import lax
from jax.experimental import pallas as pl
from jax.experimental.pallas import tpu as pltpu
from jax.sharding import PartitionSpec as P

HIGH = lax.Precision.HIGHEST
SWEEPS = 2
GROUPS = 4
DOF = 50
CHUNKS = 5
F32, BF16 = jnp.float32, jnp.bfloat16


def group_offset(group, doms):
    return [0, 1, doms // 2, doms - 1][group]


def far_first(step):
    return 4 + (step + 1) // 2 * (2 * (step % 2) - 1)


def split_dot(left, right):
    high = right.astype(BF16)
    low = (right - high.astype(F32)).astype(BF16)
    return jnp.dot(left, high, preferred_element_type=F32) + jnp.dot(
        left, low, preferred_element_type=F32
    )


def exchange_kernel(
    doms, subs,
    slot_hbm, send_hbm, recv_hbm, partner_hbm, count_hbm,
    inv_hbm, cif_hbm, cfi_hbm, ff_hbm, load_hbm, fload_hbm, jac_hbm,
    trace_ref, state_ref, faces_ref,
    jflat, jrows, sbuf, rbuf, sbig, rbig, send_sem, recv_sem, bsend_sem, brecv_sem,
    inv_ref, cif_ref, cfi_ref, ff_ref, load_ref, fload_ref, jac_ref,
    slot_ref, send_ref, recv_ref, partner_ref, count_ref, in_sem, condensed_ref, imap_ref, iload_ref, face_load_ref, blocks_ref,
    *spaces,
):
    dom, sub = lax.axis_index("dom"), lax.axis_index("sub")
    offsets = [group_offset(g, doms) for g in range(GROUPS)]
    barrier = pltpu.get_barrier_semaphore()

    def greet(step, carry):
        for g in (2, 1, 3, 0):
            other = lax.rem(sub + far_first(step), subs)
            target = lax.rem(dom + offsets[g], doms)

            def signal():
                pl.semaphore_signal(barrier, inc=1, device_id=(target, other), device_id_type=pl.DeviceIdType.MESH)

            if g == 0:
                pl.when(step < subs - 1)(signal)
            else:
                signal()
        return carry

    loads = [
        pltpu.make_async_copy(source, target, in_sem.at[k])
        for k, (source, target) in enumerate(
            (
                (inv_hbm, inv_ref), (cfi_hbm, cfi_ref), (cif_hbm, cif_ref), (ff_hbm, ff_ref),
                (load_hbm, load_ref), (fload_hbm, fload_ref), (jac_hbm, jac_ref),
                (slot_hbm, slot_ref), (send_hbm, send_ref), (recv_hbm, recv_ref),
                (partner_hbm, partner_ref), (count_hbm, count_ref),
            )
        )
    ]
    for load in loads:
        load.start()
    for phase in range(6):
        rbuf[phase] = jnp.zeros(rbuf.shape[1:], F32)
    lax.fori_loop(0, subs, greet, 0)

    condense_body(
        loads, inv_ref, cif_ref, cfi_ref, ff_ref, load_ref, fload_ref, count_ref,
        condensed_ref, imap_ref, iload_ref, face_load_ref, blocks_ref, *spaces,
    )

    loads[6].wait()
    jflat[:, 0:2500] = jac_ref[...].astype(F32)
    jflat[:, 2500:2688] = jnp.zeros((24, 188), F32)
    for i in range(DOF):
        start = DOF * i
        tile = start // 128 * 128
        window = jflat[:, tile : tile + 256] if tile + 256 <= 2688 else jflat[:, 2432:2688]
        base = tile if tile + 256 <= 2688 else 2432
        jrows[i] = pltpu.roll(window, 256 - (start - base), 1)[:, 0:128]

    lane24 = lax.broadcasted_iota(jnp.int32, (24, 128), 1)

    def jacobi(vector):
        total = jnp.zeros((24, 128), F32)
        for i in range(DOF):
            entry = jnp.sum(jrows[i] * vector, axis=1, keepdims=True)
            total = jnp.where(lane24 == i, entry, total)
        return total

    sel_a, sel_s, sel_g, sel_b, sel_r, sel_f = one_hots(slot_ref, send_ref, recv_ref, partner_ref, subs)

    pl.semaphore_wait(barrier, 31)

    def start_phase(phase, rows, sign):
        sbuf[phase] = rows

        def body(step, carry):
            other = lax.rem(sub + far_first(step), subs)
            for g in (2, 1, 3, 0):
                target = lax.rem(dom + (doms - offsets[g] if sign < 0 else offsets[g]), doms)

                def go():
                    pltpu.make_async_remote_copy(
                        src_ref=sbuf.at[phase, pl.ds(g, 1)],
                        dst_ref=rbuf.at[phase, pl.ds(g * subs + sub, 1)],
                        send_sem=send_sem.at[phase],
                        recv_sem=recv_sem.at[phase],
                        device_id=(target, other),
                        device_id_type=pl.DeviceIdType.MESH,
                    ).start()

                if g == 0:
                    pl.when(step < subs - 1)(go)
                else:
                    go()
            return carry

        lax.fori_loop(0, subs, body, 0)

    def finish_phase(phase):
        whole = rbuf.at[phase, pl.ds(0, 31)]
        pltpu.make_async_copy(whole, whole, recv_sem.at[phase]).wait()
        return rbuf[phase]

    def start_chunk(chunk):
        width = 2560 // CHUNKS

        def body(step, carry):
            other = lax.rem(sub + far_first(step), subs)
            for g in (2, 1, 3, 0):
                target = lax.rem(dom + doms - offsets[g], doms)

                def go():
                    pltpu.make_async_remote_copy(
                        src_ref=sbig.at[chunk, g],
                        dst_ref=rbig.at[chunk, g * subs + sub],
                        send_sem=bsend_sem.at[chunk],
                        recv_sem=brecv_sem.at[chunk],
                        device_id=(target, other),
                        device_id_type=pl.DeviceIdType.MESH,
                    ).start()

                if g == 0:
                    pl.when(step < subs - 1)(go)
                else:
                    go()
            return carry

        lax.fori_loop(0, subs, body, 0)

    def to_slots(wide):
        lane = lax.broadcasted_iota(jnp.int32, (8, 128), 1)
        pieces = []
        for side in range(4):
            turned = wide if side == 0 else pltpu.roll(wide, 256 - DOF * side, 1)
            pieces.append(jnp.where(lane < DOF, turned[:, 0:128], 0.0))
        return jnp.concatenate(pieces, axis=0)

    def to_elements(slots):
        zero = jnp.zeros((8, 128), F32)
        total = jnp.concatenate([slots[0:8], zero], axis=1)
        for side in range(1, 4):
            wide = jnp.concatenate([slots[8 * side : 8 * side + 8], zero], axis=1)
            total = total + pltpu.roll(wide, DOF * side, 1)
        return total

    def holder_rows(slots):
        stack = jnp.concatenate([slots, pltpu.roll(slots, 64, 1)], axis=0)
        return split_dot(sel_s[:, 0:64], stack)

    def owner_rows(traces):
        stack = jnp.concatenate([traces, pltpu.roll(traces, 64, 1)], axis=0)
        return split_dot(sel_g[:, 0:48], stack)

    def face_sum(slots, arrived):
        stack = jnp.concatenate([slots, arrived, pltpu.roll(arrived, 64, 1)], axis=0)
        total = split_dot(sel_a[:, 0:96], stack)
        return jnp.where(lane24 < DOF, total, 0.0)

    def slot_traces(traces, arrived):
        stack = jnp.concatenate([traces, arrived, pltpu.roll(arrived, 64, 1)], axis=0)
        total = split_dot(sel_b[:, 0:88], stack)
        lane = lax.broadcasted_iota(jnp.int32, (32, 128), 1)
        return jnp.where(lane < DOF, total, 0.0)

    def element_dots(elements, matrix_ref, rows):
        high = elements.astype(BF16).astype(F32)
        both = jnp.concatenate([high, elements - high], axis=0).astype(BF16)[:, 0:200]
        row = lax.broadcasted_iota(jnp.int32, (8, rows), 0)
        total = jnp.zeros((8, rows), F32)
        for e in range(8):
            out = lax.dot_general(both, matrix_ref[e], (((1,), (1,)), ((), ())), preferred_element_type=F32)
            total = jnp.where(row == e, out[0:8] + out[8:16], total)
        return total

    def wide(rows200):
        return jnp.concatenate([rows200, jnp.zeros((8, 56), F32)], axis=1)

    load_slots = to_slots(wide(face_load_ref[...]))
    start_phase(0, holder_rows(load_slots), -1)

    blocks = blocks_ref[...]
    picked = jnp.dot(sel_r[:, 0:32], blocks, preferred_element_type=F32)
    width = 2560 // CHUNKS
    for chunk in range(CHUNKS):
        for g in range(GROUPS):
            sbig[chunk, g] = picked[2 * g : 2 * g + 2, chunk * width : (chunk + 1) * width]
    start_chunk(0)
    rhs = face_sum(load_slots, finish_phase(0))
    traces = jacobi(rhs)
    for sweep in range(SWEEPS):
        start_phase(2 * sweep + 1, owner_rows(traces), 1)
        start_chunk(2 * sweep + 1)
        elements = to_elements(slot_traces(traces, finish_phase(2 * sweep + 1)))
        slots = to_slots(wide(element_dots(elements, condensed_ref, 200)))
        start_phase(2 * sweep + 2, holder_rows(slots), -1)
        start_chunk(2 * sweep + 2)
        traces = traces + jacobi(rhs - face_sum(slots, finish_phase(2 * sweep + 2)))
    start_phase(5, owner_rows(traces), 1)
    trace_ref[...] = traces
    sum_faces = jnp.dot(sel_a[:, 0:32], blocks, preferred_element_type=F32)
    for chunk in range(CHUNKS):
        pltpu.make_async_copy(rbig.at[chunk, pl.ds(0, 31)], rbig.at[chunk, pl.ds(0, 31)], brecv_sem.at[chunk]).wait()
    far = []
    for g in range(GROUPS):
        index = g * subs + partner_ref[0, g]
        far.append(jnp.concatenate([rbig[chunk, index] for chunk in range(CHUNKS)], axis=1))
    far = jnp.concatenate(far, axis=0).astype(BF16)
    sum_faces = sum_faces + jnp.dot(
        sel_f[:, 0:8], far, preferred_element_type=F32
    )
    faces_ref[...] = sum_faces
    elements = to_elements(slot_traces(traces, finish_phase(5)))
    row100 = lax.broadcasted_iota(jnp.int32, (8, 100), 0)
    state = iload_ref[...] - element_dots(elements, imap_ref, 100)
    state = jnp.where(row100 < count_ref[0], state, 0.0)
    state_ref[...] = jnp.concatenate([state, jnp.zeros((8, 28), F32)], axis=1)
    for phase in range(6):
        whole = rbuf.at[phase, pl.ds(0, 31)]
        pltpu.make_async_copy(whole, whole, send_sem.at[phase]).wait()
    for chunk in range(CHUNKS):
        whole = rbig.at[chunk, pl.ds(0, 31)]
        pltpu.make_async_copy(whole, whole, bsend_sem.at[chunk]).wait()


def one_hots(slot_ref, send_ref, recv_ref, partner_ref, subs):
    lane = lax.broadcasted_iota(jnp.int32, (8, 128), 1)
    row = lax.broadcasted_iota(jnp.int32, (8, 128), 0)
    row24 = lax.broadcasted_iota(jnp.int32, (24, 128), 0)
    row32 = lax.broadcasted_iota(jnp.int32, (32, 128), 0)
    nothing = jnp.full((8, 128), -1, jnp.int32)
    no = jnp.zeros((8, 128), F32)
    table_a, table_b, table_f, hot_s, hot_g, hot_r, local_b = nothing, nothing, nothing, no, no, no, []
    for side in range(4):
        column = nothing
        for e in range(8):
            face = slot_ref[side, e]
            face = jnp.where(face < 24, face, -1)
            table_a = jnp.where(lane == 8 * side + e, face, table_a)
            column = jnp.where(row == e, face, column)
        local_b.append((lane == column).astype(F32))
    for g in range(GROUPS):
        holder, owner = partner_ref[0, g], partner_ref[0, GROUPS + g]
        for r in range(2):
            face, slot = recv_ref[0, r, g], send_ref[0, r, g]
            face = jnp.where(face < 24, face, -1000)
            slot = jnp.where(slot < 32, (slot & 3) * 8 + (slot >> 2), -1000)
            table_a = jnp.where(lane == 32 + 32 * r + subs * g + holder, face, table_a)
            table_b = jnp.where(lane == 24 + 32 * r + subs * g + owner, slot, table_b)
            table_f = jnp.where(lane == 2 * g + r, face, table_f)
            hot_s = jnp.where((row == g) & (lane == 32 * r + slot), 1.0, hot_s)
            hot_g = jnp.where((row == g) & (lane == 24 * r + face), 1.0, hot_g)
            hot_r = jnp.where((row == 2 * g + r) & (lane == slot), 1.0, hot_r)

    def equal(rows, table):
        return (rows == jnp.concatenate([table] * (rows.shape[0] // 8), axis=0)).astype(F32)

    hot_b = equal(row32, table_b) + jnp.concatenate(local_b, axis=0)
    hots = (equal(row24, table_a), hot_s, hot_g, hot_b, hot_r, equal(row24, table_f))
    return tuple(hot.astype(BF16) for hot in hots)


def squeeze(source, flat):
    rows = source.shape[1] // 128
    for first in range(0, rows, 16):
        count = min(16, rows - first)
        line = source[0:1, 128 * first : 128 * (first + count)].astype(F32)
        flat[first : first + count, :] = line.reshape(count, 128)


def spread_rows(flat, mid, width, count, pitch):
    lane = lax.broadcasted_iota(jnp.int32, (count, 128), 1)
    for i in range(3200 // width):
        first, off = divmod(width * i, 128)
        last = (off + width - 1) // 128
        turned = []
        for tile in range(last + 1):
            value = flat[pl.ds(first + tile, count, stride=25), :]
            turned.append(pltpu.roll(value, 128 - off, 1) if off else value)
        for tile in range((width + 127) // 128):
            value = turned[tile]
            if off and tile < last:
                value = jnp.where(lane < 128 - off, value, turned[tile + 1])
            mid[tile, pl.ds(i * pitch, count), :] = value


def matrix_rows(mid, tile, first, rows, period, pitch):
    pieces = []
    for m in range(first, first + rows, 8):
        size = min(8, first + rows - m)
        p, i = divmod(m, period)
        for start, stop in ((i, min(i + size, period)), (period, i + size)):
            if stop > start:
                at = start % period * pitch + p + start // period
                pieces.append(mid[tile, pl.ds(at, stop - start, stride=pitch), :])
    return jnp.concatenate(pieces, axis=0)


def matrix(mid, e, rows, width, pitch):
    period = 3200 // width
    tiles = [matrix_rows(mid, tile, e * rows, rows, period, pitch) for tile in range((width + 127) // 128)]
    whole = tiles[0] if len(tiles) == 1 else jnp.concatenate(tiles, axis=1)
    return whole[:, 0:width]


def two_terms(rows):
    high = rows.astype(BF16).astype(F32)
    return jnp.concatenate([high, rows - high], axis=0).astype(BF16)


def times_transposed(both, right):
    out = lax.dot_general(both, right, (((1,), (1,)), ((), ())), preferred_element_type=F32)
    return out[0:8] + out[8:16]


def condense_body(
    loads, inv_ref, cif_ref, cfi_ref, ff_ref, load_ref, fload_ref, count_ref,
    condensed_ref, imap_ref, iload_ref, face_load_ref, blocks_ref,
    flat_inv, flat_cif, flat_cfi, flat_ff, mid_inv, mid_cif, mid_cfi, mid_ff, wide,
):
    loads[0].wait()
    squeeze(inv_ref, flat_inv)
    loads[1].wait()
    squeeze(cfi_ref, flat_cfi)
    spread_rows(flat_inv, mid_inv, 100, 32, 33)
    spread_rows(flat_cfi, mid_cfi, 100, 56, 57)
    loads[2].wait()
    squeeze(cif_ref, flat_cif)
    loads[3].wait()
    squeeze(ff_ref, flat_ff)
    spread_rows(flat_cif, mid_cif, 200, 56, 57)
    spread_rows(flat_ff, mid_ff, 200, 104, 105)
    for load in loads[7:]:
        load.wait()
    count = count_ref[0]
    row100 = lax.broadcasted_iota(jnp.int32, (8, 100), 0)
    row200 = lax.broadcasted_iota(jnp.int32, (8, 200), 0)
    loads[4].wait()
    loads[5].wait()
    both = two_terms(load_ref[...])
    iload = jnp.zeros((8, 100), F32)
    for e in range(8):
        inverse = matrix(mid_inv, e, 100, 100, 33).astype(BF16)
        iload = jnp.where(row100 == e, times_transposed(both, inverse), iload)
        inner = matrix(mid_cif, e, 100, 200, 57).astype(BF16)
        imap_ref[e] = jnp.dot(inverse, inner, preferred_element_type=F32).astype(BF16)
    iload_ref[...] = iload
    both = two_terms(iload)
    outer_load = jnp.zeros((8, 200), F32)
    for e in range(8):
        outer = matrix(mid_cfi, e, 200, 100, 57).astype(BF16)
        outer_load = jnp.where(row200 == e, times_transposed(both, outer), outer_load)
        product = jnp.dot(outer, imap_ref[e], preferred_element_type=F32)
        alive = jnp.where(e < count, 1.0, 0.0)
        block = ((matrix(mid_ff, e, 200, 200, 105) - product) * alive).astype(BF16)
        condensed_ref[e] = block
        block = block.astype(F32)
        wide[0, 200 * e : 200 * e + 200, :] = block[:, 0:128]
        wide[1, 200 * e : 200 * e + 200, :] = jnp.concatenate([block[:, 128:200], jnp.zeros((200, 56), F32)], axis=1)
    face_load_ref[...] = jnp.where(row200 < count, fload_ref[...] - outer_load, 0.0)

    lane = lax.broadcasted_iota(jnp.int32, (8, 128), 1)
    for side in range(4):
        start = DOF * side
        tiles = [jnp.zeros((8, 128), F32) for _ in range(20)]
        for i in range(DOF):
            at = pl.ds(start + i, 8, stride=200)
            if side == 2:
                value = jnp.where(lane < 64, wide[1, at, :], wide[0, at, :])
            else:
                value = wide[start // 128, at, :]
            tile, off = divmod(DOF * i, 128)
            shift = (off - start) % 128
            value = pltpu.roll(value, shift, 1) if shift else value
            tiles[tile] = jnp.where((lane >= off) & (lane < off + DOF), value, tiles[tile])
            if off + DOF > 128:
                tiles[tile + 1] = jnp.where(lane < off + DOF - 128, value, tiles[tile + 1])
        blocks_ref[8 * side : 8 * side + 8, :] = jnp.concatenate(tiles, axis=1).astype(BF16)


def slots_of(wide):
    lane = lax.broadcasted_iota(jnp.int32, (8, 128), 1)
    pieces = []
    for side in range(4):
        turned = wide if side == 0 else pltpu.roll(wide, 256 - DOF * side, 1)
        pieces.append(jnp.where(lane < DOF, turned[:, 0:128], 0.0))
    return jnp.concatenate(pieces, axis=0)


def elements_of(slots):
    zero = jnp.zeros((8, 128), F32)
    total = jnp.concatenate([slots[0:8], zero], axis=1)
    for side in range(1, 4):
        wide = jnp.concatenate([slots[8 * side : 8 * side + 8], zero], axis=1)
        total = total + pltpu.roll(wide, DOF * side, 1)
    return total


def each_element(elements, matrix_ref, rows):
    both = two_terms(elements)[:, 0:200]
    row = lax.broadcasted_iota(jnp.int32, (8, rows), 0)
    total = jnp.zeros((8, rows), F32)
    for e in range(8):
        total = jnp.where(row == e, times_transposed(both, matrix_ref[e]), total)
    return total


def twice(rows):
    return jnp.concatenate([rows, pltpu.roll(rows, 64, 1)], axis=0)


MIRROR = (0, 3, 2, 1)


def virtual_hots(slot_ref, send_ref, recv_ref, partner_ref, subs):
    lane = lax.broadcasted_iota(jnp.int32, (8, 128), 1)
    row = lax.broadcasted_iota(jnp.int32, (8, 128), 0)
    row24 = lax.broadcasted_iota(jnp.int32, (24, 128), 0)
    row32 = lax.broadcasted_iota(jnp.int32, (32, 128), 0)
    nothing = jnp.full((8, 128), -1000, jnp.int32)
    no = jnp.zeros((8, 128), F32)
    faces, slots = {}, {}
    for g in range(GROUPS):
        for r in range(2):
            face, slot = recv_ref[0, r, g], send_ref[0, r, g]
            faces[g, r] = jnp.where(face < 24, face, -1000)
            slots[g, r] = jnp.where(slot < 32, (slot & 3) * 8 + (slot >> 2), -1000)
    table_l, columns = nothing, []
    for side in range(4):
        column = nothing
        for e in range(8):
            face = slot_ref[side, e]
            face = jnp.where(face < 24, face, -1000)
            table_l = jnp.where(lane == 8 * side + e, face, table_l)
            column = jnp.where(row == e, face, column)
        columns.append(column)
    table_e, table_d, table_f = nothing, nothing, nothing
    hot_g, hot_r, hot_j, pick = no, no, no, [no, no]
    for g in range(GROUPS):
        holder, owner = partner_ref[0, g], partner_ref[0, GROUPS + g]
        mirror = MIRROR[g]
        for r in range(2):
            face, slot, rank = faces[g, r], slots[g, r], 24 + 2 * g + r
            table_l = jnp.where(lane == slot, rank, table_l)
            columns = [jnp.where(row + 8 * side == slot, rank, column) for side, column in enumerate(columns)]
            alive = jnp.where(slot >= 0, rank, -1000)
            table_e = jnp.where(lane == 64 * r + 2 * (subs * g + owner), alive, table_e)
            table_e = jnp.where(lane == 64 * r + 2 * (subs * mirror + holder) + 1, face, table_e)
            table_d = jnp.where(lane == 32 * r + subs * g + owner, alive, table_d)
            table_f = jnp.where(lane == 2 * g + r, face, table_f)
            hot_g = jnp.where((row == g) & (lane == 24 * r + face), 1.0, hot_g)
            hot_r = jnp.where((row == 2 * g + r) & (lane == slot), 1.0, hot_r)
            hot_j = jnp.where((row == 2 * g + r) & (lane == face), 1.0, hot_j)
            pick[r] = jnp.where((row == 2 * g) & (lane == face), 1.0, pick[r])
            pick[r] = jnp.where((row == 2 * mirror + 1) & (lane == rank), 1.0, pick[r])

    def equal(rows, table):
        return (rows == jnp.concatenate([table] * (rows.shape[0] // 8), axis=0)).astype(F32)

    hot_x = jnp.concatenate([(lane == column).astype(F32) for column in columns], axis=0)
    local = equal(row32, table_l).astype(BF16)
    sent = [jnp.dot(part.astype(BF16)[:, 0:32], local, preferred_element_type=F32) for part in pick]
    hot_s = sent[0] + pltpu.roll(sent[1], 32, 1)
    twins = jnp.int32(0)
    flat = [faces[g, r] for g in range(GROUPS) for r in range(2)]
    for k, face in enumerate(flat):
        for other in flat[:k]:
            twins = twins + jnp.where(face == other, jnp.where(face >= 0, 1, 0), 0)
    hots = (hot_s, hot_x, equal(row32, table_e), equal(row32, table_d), hot_g, hot_r, hot_j, equal(row24, table_f))
    return (local,) + tuple(hot.astype(BF16) for hot in hots) + (twins,)


def sweep_kernel(
    doms, subs,
    slot_hbm, send_hbm, recv_hbm, partner_hbm, count_hbm,
    inv_hbm, cif_hbm, cfi_hbm, ff_hbm, load_hbm, fload_hbm, jac_hbm,
    trace_ref, state_ref, faces_ref, twins_ref,
    jflat, jrows, esend, ebuf, dsend, dbuf, fsend, fbuf, bsend, bbuf, jsend, jbuf,
    esend_sem, erecv_sem, dsend_sem, drecv_sem, fsend_sem, frecv_sem, bsend_sem, brecv_sem, jsend_sem, jrecv_sem,
    inv_ref, cif_ref, cfi_ref, ff_ref, load_ref, fload_ref, jac_ref,
    slot_ref, send_ref, recv_ref, partner_ref, count_ref, in_sem,
    condensed_ref, imap_ref, iload_ref, face_load_ref, blocks_ref,
    *spaces,
):
    dom, sub = lax.axis_index("dom"), lax.axis_index("sub")
    mesh_ids = pl.DeviceIdType.MESH
    offsets = [group_offset(g, doms) for g in range(GROUPS)]
    barrier = pltpu.get_barrier_semaphore()
    rank, block = lax.rem(dom, 8), dom // 8

    def hello(target, other):
        pl.semaphore_signal(barrier, inc=1, device_id=(target, other), device_id_type=mesh_ids)

    def to_all(start):
        def body(step, carry):
            other = lax.rem(sub + far_first(step), subs)
            for g in (2, 1, 3, 0):
                target = lax.rem(dom + offsets[g], doms)
                if g == 0:
                    pl.when(step < subs - 1)(functools.partial(start, g, target, other))
                else:
                    start(g, target, other)
            return carry

        lax.fori_loop(0, subs, body, 0)

    stages = (
        lambda step: (dom, lax.rem(sub + step, subs)),
        lambda step: (lax.rem(dom + 8 * step, doms), sub),
        lambda step: (8 * block + lax.rem(rank + step, 8), sub),
    )
    places = (sub, block, rank)
    for phase in range(3):
        ebuf[phase] = jnp.zeros(ebuf.shape[1:], F32)
        fbuf[phase] = jnp.zeros(fbuf.shape[1:], F32)
    dbuf[...] = jnp.zeros(dbuf.shape, F32)
    to_all(lambda g, target, other: hello(target, other))

    def more(step, carry):
        hello(*stages[1](step))
        hello(*stages[2](step))
        return carry

    lax.fori_loop(1, 8, more, 0)
    loads = [
        pltpu.make_async_copy(source, target, in_sem.at[k])
        for k, (source, target) in enumerate(
            (
                (inv_hbm, inv_ref), (cfi_hbm, cfi_ref), (cif_hbm, cif_ref), (ff_hbm, ff_ref),
                (load_hbm, load_ref), (fload_hbm, fload_ref), (jac_hbm, jac_ref),
                (slot_hbm, slot_ref), (send_hbm, send_ref), (recv_hbm, recv_ref),
                (partner_hbm, partner_ref), (count_hbm, count_ref),
            )
        )
    ]
    for load in loads:
        load.start()
    condense_body(
        loads, inv_ref, cif_ref, cfi_ref, ff_ref, load_ref, fload_ref, count_ref,
        condensed_ref, imap_ref, iload_ref, face_load_ref, blocks_ref, *spaces,
    )
    local, hot_s, hot_x, hot_e, hot_d, hot_g, hot_r, hot_j, hot_f, twins = virtual_hots(
        slot_ref, send_ref, recv_ref, partner_ref, subs
    )

    def fill_rows(first, rows):
        for i in range(DOF):
            start = DOF * i
            base = min(start // 128 * 128, 2432)
            window = jflat[first : first + rows, base : base + 256]
            jrows[i, first : first + rows, :] = pltpu.roll(window, 256 - (start - base), 1)[:, 0:128]

    loads[6].wait()
    jflat[0:24, 0:2500] = jac_ref[...].astype(F32)
    jflat[:, 2500:2688] = jnp.zeros((32, 188), F32)
    jflat[24:32, 0:2500] = jnp.zeros((8, 2500), F32)
    for i in range(DOF):
        jrows[i, 24:32, :] = jnp.zeros((8, 128), F32)
    fill_rows(0, 24)
    part = 2560 // CHUNKS
    inverses = jflat[0:24, 0:2560].astype(BF16)
    blocks = blocks_ref[...]
    picked_j = jnp.dot(hot_j[:, 0:24], inverses, preferred_element_type=F32)
    picked_b = jnp.dot(hot_r[:, 0:32], blocks, preferred_element_type=F32)
    for chunk in range(CHUNKS):
        for g in range(GROUPS):
            jsend[chunk, g] = picked_j[2 * g : 2 * g + 2, chunk * part : (chunk + 1) * part]
            bsend[chunk, MIRROR[g]] = picked_b[2 * g : 2 * g + 2, chunk * part : (chunk + 1) * part]
    lane32 = lax.broadcasted_iota(jnp.int32, (32, 128), 1)

    def short(rows):
        return jnp.where(lane32 < DOF, rows, 0.0)

    def jacobi(vector):
        total = jnp.zeros((32, 128), F32)
        for i in range(DOF):
            entry = jnp.sum(jrows[i] * vector, axis=1, keepdims=True)
            total = jnp.where(lane32 == i, entry, total)
        return total

    def start_swap(phase, slots):
        esend[phase] = split_dot(hot_s[:, 0:64], twice(slots))

        def start(g, target, other):
            pltpu.make_async_remote_copy(
                src_ref=esend.at[phase, pl.ds(2 * g, 2)],
                dst_ref=ebuf.at[phase, pl.ds(2 * (g * subs + sub), 2)],
                send_sem=esend_sem.at[phase], recv_sem=erecv_sem.at[phase],
                device_id=(target, other), device_id_type=mesh_ids,
            ).start()

        to_all(start)

    def finish_swap(phase, slots):
        own = split_dot(local[:, 0:32], slots)
        whole = ebuf.at[phase, pl.ds(0, 62)]
        pltpu.make_async_copy(whole, whole, erecv_sem.at[phase]).wait()
        return short(own + split_dot(hot_e, twice(ebuf[phase])))

    def start_stage(stage, value):
        fsend[stage] = value

        def body(step, carry):
            pltpu.make_async_remote_copy(
                src_ref=fsend.at[stage, pl.ds(0, 1)], dst_ref=fbuf.at[stage, pl.ds(places[stage], 1)],
                send_sem=fsend_sem.at[stage], recv_sem=frecv_sem.at[stage],
                device_id=stages[stage](step), device_id_type=mesh_ids,
            ).start()
            return carry

        lax.fori_loop(1, 8, body, 0)

    def finish_stage(stage, value):
        whole = fbuf.at[stage, pl.ds(0, 7)]
        pltpu.make_async_copy(whole, whole, frecv_sem.at[stage]).wait()
        return value + jnp.sum(fbuf[stage], axis=0, keepdims=True)

    def start_chunks(source, target_ref, send_sem, recv_sem, first, last):
        for chunk in range(first, last):

            def start(g, target, other):
                pltpu.make_async_remote_copy(
                    src_ref=source.at[chunk, g], dst_ref=target_ref.at[chunk, g * subs + sub],
                    send_sem=send_sem.at[chunk], recv_sem=recv_sem.at[chunk],
                    device_id=(target, other), device_id_type=mesh_ids,
                ).start()

            to_all(start)

    def finish_chunks(target_ref, recv_sem, index):
        for chunk in range(CHUNKS):
            whole = target_ref.at[chunk, pl.ds(0, 31)]
            pltpu.make_async_copy(whole, whole, recv_sem.at[chunk]).wait()
        rows = [
            jnp.concatenate([target_ref[chunk, index(g)] for chunk in range(CHUNKS)], axis=1) for g in range(GROUPS)
        ]
        return jnp.concatenate(rows, axis=0)

    start_jac = functools.partial(start_chunks, jsend, jbuf, jsend_sem, jrecv_sem)
    start_blocks = functools.partial(start_chunks, bsend, bbuf, bsend_sem, brecv_sem)
    found = jnp.zeros((8, 128), F32) + twins.astype(F32)

    def padded(rows):
        return jnp.concatenate([rows, jnp.zeros((8, 56), F32)], axis=1)

    slots = slots_of(padded(face_load_ref[...]))
    pl.semaphore_wait(barrier, 45)
    start_swap(0, slots)
    start_stage(0, found)
    start_jac(0, 3)
    rhs = finish_swap(0, slots)
    found = finish_stage(0, found)
    traces = jacobi(rhs)

    dsend[...] = split_dot(hot_g[:, 0:48], twice(traces[0:24]))

    def start_trace(g, target, other):
        pltpu.make_async_remote_copy(
            src_ref=dsend.at[pl.ds(g, 1)], dst_ref=dbuf.at[pl.ds(g * subs + sub, 1)],
            send_sem=dsend_sem, recv_sem=drecv_sem, device_id=(target, other), device_id_type=mesh_ids,
        ).start()

    to_all(start_trace)
    start_stage(1, found)
    start_jac(3, 5)
    start_blocks(0, 1)
    pltpu.make_async_copy(dbuf.at[pl.ds(0, 31)], dbuf.at[pl.ds(0, 31)], drecv_sem).wait()
    traces = short(traces + split_dot(hot_d[:, 0:64], twice(dbuf[...])))
    found = finish_stage(1, found)

    for sweep in range(SWEEPS):
        elements = elements_of(short(split_dot(hot_x[:, 0:32], traces)))
        slots = slots_of(padded(each_element(elements, condensed_ref, 200)))
        start_swap(1 + sweep, slots)
        start_blocks(1 + 2 * sweep, 3 + 2 * sweep)
        if sweep == 0:
            start_stage(2, found)
        total = finish_swap(1 + sweep, slots)
        if sweep == 0:
            jflat[24:32, 0:2560] = finish_chunks(jbuf, jrecv_sem, lambda g: g * subs + partner_ref[0, GROUPS + g])
            fill_rows(24, 8)
        traces = traces + jacobi(rhs - total)
    twins_ref[...] = jnp.where(finish_stage(2, found)[0:1, 0:1] > 0.0, 1, 0)
    trace_ref[...] = traces[0:24]
    elements = elements_of(short(split_dot(hot_x[:, 0:32], traces)))
    row100 = lax.broadcasted_iota(jnp.int32, (8, 100), 0)
    state = iload_ref[...] - each_element(elements, imap_ref, 100)
    state = jnp.where(row100 < count_ref[0], state, 0.0)
    state_ref[...] = jnp.concatenate([state, jnp.zeros((8, 28), F32)], axis=1)
    sums = jnp.dot(local[0:24, 0:32], blocks, preferred_element_type=F32)
    far = finish_chunks(bbuf, brecv_sem, lambda g: MIRROR[g] * subs + partner_ref[0, g]).astype(BF16)
    faces_ref[...] = sums + jnp.dot(hot_f[:, 0:8], far, preferred_element_type=F32)
    for phase in range(3):
        pltpu.make_async_copy(ebuf.at[phase, pl.ds(0, 62)], ebuf.at[phase, pl.ds(0, 62)], esend_sem.at[phase]).wait()
        pltpu.make_async_copy(fbuf.at[phase, pl.ds(0, 7)], fbuf.at[phase, pl.ds(0, 7)], fsend_sem.at[phase]).wait()
    pltpu.make_async_copy(dbuf.at[pl.ds(0, 31)], dbuf.at[pl.ds(0, 31)], dsend_sem).wait()
    for chunk in range(CHUNKS):
        whole = bbuf.at[chunk, pl.ds(0, 31)]
        pltpu.make_async_copy(whole, whole, bsend_sem.at[chunk]).wait()
        whole = jbuf.at[chunk, pl.ds(0, 31)]
        pltpu.make_async_copy(whole, whole, jsend_sem.at[chunk]).wait()


def finish_kernel(trace_ref, state_ref, faces_ref, trace_out, state_out, faces_out):
    trace_out[...] = trace_ref[:, 0:DOF]
    state_out[...] = state_ref[:, 0:100]
    faces_out[...] = faces_ref[:, 0 : DOF * DOF].astype(BF16)


def six_exchanges(
    doms, subs,
    inv_interior, couple_if, couple_fi, face_face, load_interior, load_face, jacobi_inverse,
    slot_face, send_slot, recv_face, partner_sub, elem_count,
):
    vmem = pl.BlockSpec(memory_space=pltpu.VMEM)
    part = 2560 // CHUNKS
    results = pl.pallas_call(
        functools.partial(exchange_kernel, doms, subs),
        out_shape=(
            jax.ShapeDtypeStruct((24, 128), F32),
            jax.ShapeDtypeStruct((8, 128), F32),
            jax.ShapeDtypeStruct((24, 2560), F32),
        ),
        in_specs=[pl.BlockSpec(memory_space=pl.ANY)] * 12,
        out_specs=(vmem, vmem, vmem),
        scratch_shapes=[
            pltpu.VMEM((24, 2688), F32),
            pltpu.VMEM((DOF, 24, 128), F32),
            pltpu.VMEM((6, 8, 128), F32),
            pltpu.VMEM((6, 32, 128), F32),
            pltpu.VMEM((CHUNKS, GROUPS, 2, part), F32),
            pltpu.VMEM((CHUNKS, 32, 2, part), F32),
            pltpu.SemaphoreType.DMA((6,)),
            pltpu.SemaphoreType.DMA((6,)),
            pltpu.SemaphoreType.DMA((CHUNKS,)),
            pltpu.SemaphoreType.DMA((CHUNKS,)),
        ] + local_scratch(inv_interior, couple_if, couple_fi, face_face),
        compiler_params=pltpu.CompilerParams(collective_id=1, has_side_effects=True),
    )(
        slot_face.T, send_slot.transpose(0, 2, 1), recv_face.transpose(0, 2, 1), partner_sub, elem_count,
        inv_interior, couple_if, couple_fi, face_face, load_interior, load_face, jacobi_inverse,
    )
    return finish(results)


def local_scratch(inv_interior, couple_if, couple_fi, face_face):
    return [
        pltpu.VMEM(inv_interior.shape, BF16),
        pltpu.VMEM(couple_if.shape, BF16),
        pltpu.VMEM(couple_fi.shape, BF16),
        pltpu.VMEM(face_face.shape, BF16),
        pltpu.VMEM((8, 100), F32),
        pltpu.VMEM((8, 200), F32),
        pltpu.VMEM((24, 2500), BF16),
        pltpu.SMEM((4, 8), jnp.int32),
        pltpu.SMEM((1, 2, 4), jnp.int32),
        pltpu.SMEM((1, 2, 4), jnp.int32),
        pltpu.SMEM((1, 8), jnp.int32),
        pltpu.SMEM((1,), jnp.int32),
        pltpu.SemaphoreType.DMA((12,)),
        pltpu.VMEM((8, 200, 200), BF16),
        pltpu.VMEM((8, 100, 200), BF16),
        pltpu.VMEM((8, 100), F32),
        pltpu.VMEM((8, 200), F32),
        pltpu.VMEM((32, 2560), BF16),
        pltpu.VMEM((808, 128), F32),
        pltpu.VMEM((1408, 128), F32),
        pltpu.VMEM((1408, 128), F32),
        pltpu.VMEM((2608, 128), F32),
        pltpu.VMEM((1, 1064, 128), F32),
        pltpu.VMEM((2, 920, 128), F32),
        pltpu.VMEM((1, 1832, 128), F32),
        pltpu.VMEM((2, 1688, 128), F32),
        pltpu.VMEM((2, 1600, 128), F32),
    ]


def finish(results):
    vmem = pl.BlockSpec(memory_space=pltpu.VMEM)
    return pl.pallas_call(
        finish_kernel,
        out_shape=(
            jax.ShapeDtypeStruct((24, DOF), F32),
            jax.ShapeDtypeStruct((8, 100), F32),
            jax.ShapeDtypeStruct((24, DOF * DOF), BF16),
        ),
        in_specs=[vmem] * 3,
        out_specs=(vmem, vmem, vmem),
    )(*results)


def per_device(doms, subs, *arrays):
    vmem = pl.BlockSpec(memory_space=pltpu.VMEM)
    part = 2560 // CHUNKS
    loads, tables = arrays[:7], arrays[7:]
    slot_face, send_slot, recv_face, partner_sub, elem_count = tables
    *results, twins = pl.pallas_call(
        functools.partial(sweep_kernel, doms, subs),
        out_shape=(
            jax.ShapeDtypeStruct((24, 128), F32),
            jax.ShapeDtypeStruct((8, 128), F32),
            jax.ShapeDtypeStruct((24, 2560), F32),
            jax.ShapeDtypeStruct((1, 1), jnp.int32),
        ),
        in_specs=[pl.BlockSpec(memory_space=pl.ANY)] * 12,
        out_specs=(vmem, vmem, vmem, vmem),
        scratch_shapes=[
            pltpu.VMEM((32, 2688), F32),
            pltpu.VMEM((DOF, 32, 128), F32),
            pltpu.VMEM((3, 8, 128), F32),
            pltpu.VMEM((3, 64, 128), F32),
            pltpu.VMEM((8, 128), F32),
            pltpu.VMEM((32, 128), F32),
            pltpu.VMEM((3, 8, 128), F32),
            pltpu.VMEM((3, 8, 128), F32),
            pltpu.VMEM((CHUNKS, GROUPS, 2, part), F32),
            pltpu.VMEM((CHUNKS, 32, 2, part), F32),
            pltpu.VMEM((CHUNKS, GROUPS, 2, part), F32),
            pltpu.VMEM((CHUNKS, 32, 2, part), F32),
            pltpu.SemaphoreType.DMA((3,)),
            pltpu.SemaphoreType.DMA((3,)),
            pltpu.SemaphoreType.DMA,
            pltpu.SemaphoreType.DMA,
            pltpu.SemaphoreType.DMA((3,)),
            pltpu.SemaphoreType.DMA((3,)),
            pltpu.SemaphoreType.DMA((CHUNKS,)),
            pltpu.SemaphoreType.DMA((CHUNKS,)),
            pltpu.SemaphoreType.DMA((CHUNKS,)),
            pltpu.SemaphoreType.DMA((CHUNKS,)),
        ] + local_scratch(*loads[:4]),
        compiler_params=pltpu.CompilerParams(collective_id=0, has_side_effects=True, vmem_limit_bytes=67043328),
    )(slot_face.T, send_slot.transpose(0, 2, 1), recv_face.transpose(0, 2, 1), partner_sub, elem_count, *loads)
    return lax.switch(
        twins.reshape(()),
        (lambda: finish(results), lambda: six_exchanges(doms, subs, *arrays)),
    )


def solution(mesh):
    rows = P(("dom", "sub"), None)
    placed = (rows,) * 8 + (P(("dom", "sub"), None, None),) * 2 + (rows, P(("dom", "sub")))
    return jax.shard_map(
        functools.partial(per_device, mesh.shape["dom"], mesh.shape["sub"]),
        mesh=mesh,
        in_specs=placed,
        out_specs=(rows, rows, rows),
        check_vma=False,
    )
```

```python
import functools

import jax
import jax.numpy as jnp
from jax import lax
from jax.experimental import pallas as pl
from jax.experimental.pallas import tpu as pltpu
from jax.sharding import PartitionSpec as P

HIGH = lax.Precision.HIGHEST
SWEEPS = 2
GROUPS = 4
DOF = 50
CHUNKS = 5
F32, BF16 = jnp.float32, jnp.bfloat16


def group_offset(group, doms):
    return [0, 1, doms // 2, doms - 1][group]


def far_first(step):
    return 4 + (step + 1) // 2 * (2 * (step % 2) - 1)


def split_dot(left, right):
    high = right.astype(BF16)
    low = (right - high.astype(F32)).astype(BF16)
    return jnp.dot(left, high, preferred_element_type=F32) + jnp.dot(
        left, low, preferred_element_type=F32
    )


def exchange_kernel(
    doms, subs,
    slot_hbm, send_hbm, recv_hbm, partner_hbm, count_hbm,
    inv_hbm, cif_hbm, cfi_hbm, ff_hbm, load_hbm, fload_hbm, jac_hbm,
    trace_ref, state_ref, faces_ref,
    jflat, jrows, sbuf, rbuf, sbig, rbig, send_sem, recv_sem, bsend_sem, brecv_sem,
    inv_ref, cif_ref, cfi_ref, ff_ref, load_ref, fload_ref, jac_ref,
    slot_ref, send_ref, recv_ref, partner_ref, count_ref, in_sem, condensed_ref, imap_ref, iload_ref, face_load_ref, blocks_ref,
    *spaces,
):
    dom, sub = lax.axis_index("dom"), lax.axis_index("sub")
    offsets = [group_offset(g, doms) for g in range(GROUPS)]
    barrier = pltpu.get_barrier_semaphore()

    def greet(step, carry):
        for g in (2, 1, 3, 0):
            other = lax.rem(sub + far_first(step), subs)
            target = lax.rem(dom + offsets[g], doms)

            def signal():
                pl.semaphore_signal(barrier, inc=1, device_id=(target, other), device_id_type=pl.DeviceIdType.MESH)

            if g == 0:
                pl.when(step < subs - 1)(signal)
            else:
                signal()
        return carry

    loads = [
        pltpu.make_async_copy(source, target, in_sem.at[k])
        for k, (source, target) in enumerate(
            (
                (inv_hbm, inv_ref), (cfi_hbm, cfi_ref), (cif_hbm, cif_ref), (ff_hbm, ff_ref),
                (load_hbm, load_ref), (fload_hbm, fload_ref), (jac_hbm, jac_ref),
                (slot_hbm, slot_ref), (send_hbm, send_ref), (recv_hbm, recv_ref),
                (partner_hbm, partner_ref), (count_hbm, count_ref),
            )
        )
    ]
    for load in loads:
        load.start()
    for phase in range(6):
        rbuf[phase] = jnp.zeros(rbuf.shape[1:], F32)
    lax.fori_loop(0, subs, greet, 0)

    condense_body(
        loads, inv_ref, cif_ref, cfi_ref, ff_ref, load_ref, fload_ref, count_ref,
        condensed_ref, imap_ref, iload_ref, face_load_ref, blocks_ref, *spaces,
    )

    loads[6].wait()
    jflat[:, 0:2500] = jac_ref[...].astype(F32)
    jflat[:, 2500:2688] = jnp.zeros((24, 188), F32)
    for i in range(DOF):
        start = DOF * i
        tile = start // 128 * 128
        window = jflat[:, tile : tile + 256] if tile + 256 <= 2688 else jflat[:, 2432:2688]
        base = tile if tile + 256 <= 2688 else 2432
        jrows[i] = pltpu.roll(window, 256 - (start - base), 1)[:, 0:128]

    lane24 = lax.broadcasted_iota(jnp.int32, (24, 128), 1)

    def jacobi(vector):
        total = jnp.zeros((24, 128), F32)
        for i in range(DOF):
            entry = jnp.sum(jrows[i] * vector, axis=1, keepdims=True)
            total = jnp.where(lane24 == i, entry, total)
        return total

    sel_a, sel_s, sel_g, sel_b, sel_r, sel_f = one_hots(slot_ref, send_ref, recv_ref, partner_ref, subs)

    pl.semaphore_wait(barrier, 31)

    def start_phase(phase, rows, sign):
        sbuf[phase] = rows

        def body(step, carry):
            other = lax.rem(sub + far_first(step), subs)
            for g in (2, 1, 3, 0):
                target = lax.rem(dom + (doms - offsets[g] if sign < 0 else offsets[g]), doms)

                def go():
                    pltpu.make_async_remote_copy(
                        src_ref=sbuf.at[phase, pl.ds(g, 1)],
                        dst_ref=rbuf.at[phase, pl.ds(g * subs + sub, 1)],
                        send_sem=send_sem.at[phase],
                        recv_sem=recv_sem.at[phase],
                        device_id=(target, other),
                        device_id_type=pl.DeviceIdType.MESH,
                    ).start()

                if g == 0:
                    pl.when(step < subs - 1)(go)
                else:
                    go()
            return carry

        lax.fori_loop(0, subs, body, 0)

    def finish_phase(phase):
        whole = rbuf.at[phase, pl.ds(0, 31)]
        pltpu.make_async_copy(whole, whole, recv_sem.at[phase]).wait()
        return rbuf[phase]

    def start_chunk(chunk):
        width = 2560 // CHUNKS

        def body(step, carry):
            other = lax.rem(sub + far_first(step), subs)
            for g in (2, 1, 3, 0):
                target = lax.rem(dom + doms - offsets[g], doms)

                def go():
                    pltpu.make_async_remote_copy(
                        src_ref=sbig.at[chunk, g],
                        dst_ref=rbig.at[chunk, g * subs + sub],
                        send_sem=bsend_sem.at[chunk],
                        recv_sem=brecv_sem.at[chunk],
                        device_id=(target, other),
                        device_id_type=pl.DeviceIdType.MESH,
                    ).start()

                if g == 0:
                    pl.when(step < subs - 1)(go)
                else:
                    go()
            return carry

        lax.fori_loop(0, subs, body, 0)

    def to_slots(wide):
        lane = lax.broadcasted_iota(jnp.int32, (8, 128), 1)
        pieces = []
        for side in range(4):
            turned = wide if side == 0 else pltpu.roll(wide, 256 - DOF * side, 1)
            pieces.append(jnp.where(lane < DOF, turned[:, 0:128], 0.0))
        return jnp.concatenate(pieces, axis=0)

    def to_elements(slots):
        zero = jnp.zeros((8, 128), F32)
        total = jnp.concatenate([slots[0:8], zero], axis=1)
        for side in range(1, 4):
            wide = jnp.concatenate([slots[8 * side : 8 * side + 8], zero], axis=1)
            total = total + pltpu.roll(wide, DOF * side, 1)
        return total

    def holder_rows(slots):
        stack = jnp.concatenate([slots, pltpu.roll(slots, 64, 1)], axis=0)
        return split_dot(sel_s[:, 0:64], stack)

    def owner_rows(traces):
        stack = jnp.concatenate([traces, pltpu.roll(traces, 64, 1)], axis=0)
        return split_dot(sel_g[:, 0:48], stack)

    def face_sum(slots, arrived):
        stack = jnp.concatenate([slots, arrived, pltpu.roll(arrived, 64, 1)], axis=0)
        total = split_dot(sel_a[:, 0:96], stack)
        return jnp.where(lane24 < DOF, total, 0.0)

    def slot_traces(traces, arrived):
        stack = jnp.concatenate([traces, arrived, pltpu.roll(arrived, 64, 1)], axis=0)
        total = split_dot(sel_b[:, 0:88], stack)
        lane = lax.broadcasted_iota(jnp.int32, (32, 128), 1)
        return jnp.where(lane < DOF, total, 0.0)

    def element_dots(elements, matrix_ref, rows):
        high = elements.astype(BF16).astype(F32)
        both = jnp.concatenate([high, elements - high], axis=0).astype(BF16)[:, 0:200]
        row = lax.broadcasted_iota(jnp.int32, (8, rows), 0)
        total = jnp.zeros((8, rows), F32)
        for e in range(8):
            out = lax.dot_general(both, matrix_ref[e], (((1,), (1,)), ((), ())), preferred_element_type=F32)
            total = jnp.where(row == e, out[0:8] + out[8:16], total)
        return total

    def wide(rows200):
        return jnp.concatenate([rows200, jnp.zeros((8, 56), F32)], axis=1)

    load_slots = to_slots(wide(face_load_ref[...]))
    start_phase(0, holder_rows(load_slots), -1)

    blocks = blocks_ref[...]
    picked = jnp.dot(sel_r[:, 0:32], blocks, preferred_element_type=F32)
    width = 2560 // CHUNKS
    for chunk in range(CHUNKS):
        for g in range(GROUPS):
            sbig[chunk, g] = picked[2 * g : 2 * g + 2, chunk * width : (chunk + 1) * width]
    start_chunk(0)
    rhs = face_sum(load_slots, finish_phase(0))
    traces = jacobi(rhs)
    for sweep in range(SWEEPS):
        start_phase(2 * sweep + 1, owner_rows(traces), 1)
        start_chunk(2 * sweep + 1)
        elements = to_elements(slot_traces(traces, finish_phase(2 * sweep + 1)))
        slots = to_slots(wide(element_dots(elements, condensed_ref, 200)))
        start_phase(2 * sweep + 2, holder_rows(slots), -1)
        start_chunk(2 * sweep + 2)
        traces = traces + jacobi(rhs - face_sum(slots, finish_phase(2 * sweep + 2)))
    start_phase(5, owner_rows(traces), 1)
    trace_ref[...] = traces
    sum_faces = jnp.dot(sel_a[:, 0:32], blocks, preferred_element_type=F32)
    for chunk in range(CHUNKS):
        pltpu.make_async_copy(rbig.at[chunk, pl.ds(0, 31)], rbig.at[chunk, pl.ds(0, 31)], brecv_sem.at[chunk]).wait()
    far = []
    for g in range(GROUPS):
        index = g * subs + partner_ref[0, g]
        far.append(jnp.concatenate([rbig[chunk, index] for chunk in range(CHUNKS)], axis=1))
    far = jnp.concatenate(far, axis=0).astype(BF16)
    sum_faces = sum_faces + jnp.dot(
        sel_f[:, 0:8], far, preferred_element_type=F32
    )
    faces_ref[...] = sum_faces
    elements = to_elements(slot_traces(traces, finish_phase(5)))
    row100 = lax.broadcasted_iota(jnp.int32, (8, 100), 0)
    state = iload_ref[...] - element_dots(elements, imap_ref, 100)
    state = jnp.where(row100 < count_ref[0], state, 0.0)
    state_ref[...] = jnp.concatenate([state, jnp.zeros((8, 28), F32)], axis=1)
    for phase in range(6):
        whole = rbuf.at[phase, pl.ds(0, 31)]
        pltpu.make_async_copy(whole, whole, send_sem.at[phase]).wait()
    for chunk in range(CHUNKS):
        whole = rbig.at[chunk, pl.ds(0, 31)]
        pltpu.make_async_copy(whole, whole, bsend_sem.at[chunk]).wait()


def one_hots(slot_ref, send_ref, recv_ref, partner_ref, subs):
    lane = lax.broadcasted_iota(jnp.int32, (8, 128), 1)
    row = lax.broadcasted_iota(jnp.int32, (8, 128), 0)
    row24 = lax.broadcasted_iota(jnp.int32, (24, 128), 0)
    row32 = lax.broadcasted_iota(jnp.int32, (32, 128), 0)
    nothing = jnp.full((8, 128), -1, jnp.int32)
    no = jnp.zeros((8, 128), F32)
    table_a, table_b, table_f, hot_s, hot_g, hot_r, local_b = nothing, nothing, nothing, no, no, no, []
    for side in range(4):
        column = nothing
        for e in range(8):
            face = slot_ref[side, e]
            face = jnp.where(face < 24, face, -1)
            table_a = jnp.where(lane == 8 * side + e, face, table_a)
            column = jnp.where(row == e, face, column)
        local_b.append((lane == column).astype(F32))
    for g in range(GROUPS):
        holder, owner = partner_ref[0, g], partner_ref[0, GROUPS + g]
        for r in range(2):
            face, slot = recv_ref[0, r, g], send_ref[0, r, g]
            face = jnp.where(face < 24, face, -1000)
            slot = jnp.where(slot < 32, (slot & 3) * 8 + (slot >> 2), -1000)
            table_a = jnp.where(lane == 32 + 32 * r + subs * g + holder, face, table_a)
            table_b = jnp.where(lane == 24 + 32 * r + subs * g + owner, slot, table_b)
            table_f = jnp.where(lane == 2 * g + r, face, table_f)
            hot_s = jnp.where((row == g) & (lane == 32 * r + slot), 1.0, hot_s)
            hot_g = jnp.where((row == g) & (lane == 24 * r + face), 1.0, hot_g)
            hot_r = jnp.where((row == 2 * g + r) & (lane == slot), 1.0, hot_r)

    def equal(rows, table):
        return (rows == jnp.concatenate([table] * (rows.shape[0] // 8), axis=0)).astype(F32)

    hot_b = equal(row32, table_b) + jnp.concatenate(local_b, axis=0)
    hots = (equal(row24, table_a), hot_s, hot_g, hot_b, hot_r, equal(row24, table_f))
    return tuple(hot.astype(BF16) for hot in hots)


def squeeze(source, flat):
    rows = source.shape[1] // 128
    for first in range(0, rows, 16):
        count = min(16, rows - first)
        line = source[0:1, 128 * first : 128 * (first + count)].astype(F32)
        flat[first : first + count, :] = line.reshape(count, 128)


def spread_rows(flat, mid, width, count, pitch):
    lane = lax.broadcasted_iota(jnp.int32, (count, 128), 1)
    for i in range(3200 // width):
        first, off = divmod(width * i, 128)
        last = (off + width - 1) // 128
        turned = []
        for tile in range(last + 1):
            value = flat[pl.ds(first + tile, count, stride=25), :]
            turned.append(pltpu.roll(value, 128 - off, 1) if off else value)
        for tile in range((width + 127) // 128):
            value = turned[tile]
            if off and tile < last:
                value = jnp.where(lane < 128 - off, value, turned[tile + 1])
            mid[tile, pl.ds(i * pitch, count), :] = value


def matrix_rows(mid, tile, first, rows, period, pitch):
    pieces = []
    for m in range(first, first + rows, 8):
        size = min(8, first + rows - m)
        p, i = divmod(m, period)
        for start, stop in ((i, min(i + size, period)), (period, i + size)):
            if stop > start:
                at = start % period * pitch + p + start // period
                pieces.append(mid[tile, pl.ds(at, stop - start, stride=pitch), :])
    return jnp.concatenate(pieces, axis=0)


def matrix(mid, e, rows, width, pitch):
    period = 3200 // width
    tiles = [matrix_rows(mid, tile, e * rows, rows, period, pitch) for tile in range((width + 127) // 128)]
    whole = tiles[0] if len(tiles) == 1 else jnp.concatenate(tiles, axis=1)
    return whole[:, 0:width]


def two_terms(rows):
    high = rows.astype(BF16).astype(F32)
    return jnp.concatenate([high, rows - high], axis=0).astype(BF16)


def times_transposed(both, right):
    out = lax.dot_general(both, right, (((1,), (1,)), ((), ())), preferred_element_type=F32)
    return out[0:8] + out[8:16]


def condense_body(
    loads, inv_ref, cif_ref, cfi_ref, ff_ref, load_ref, fload_ref, count_ref,
    condensed_ref, imap_ref, iload_ref, face_load_ref, blocks_ref,
    flat_inv, flat_cif, flat_cfi, flat_ff, mid_inv, mid_cif, mid_cfi, mid_ff, wide,
):
    loads[0].wait()
    squeeze(inv_ref, flat_inv)
    loads[1].wait()
    squeeze(cfi_ref, flat_cfi)
    spread_rows(flat_inv, mid_inv, 100, 32, 33)
    spread_rows(flat_cfi, mid_cfi, 100, 56, 57)
    loads[2].wait()
    squeeze(cif_ref, flat_cif)
    loads[3].wait()
    squeeze(ff_ref, flat_ff)
    spread_rows(flat_cif, mid_cif, 200, 56, 57)
    spread_rows(flat_ff, mid_ff, 200, 104, 105)
    for load in loads[7:]:
        load.wait()
    count = count_ref[0]
    row100 = lax.broadcasted_iota(jnp.int32, (8, 100), 0)
    row200 = lax.broadcasted_iota(jnp.int32, (8, 200), 0)
    loads[4].wait()
    loads[5].wait()
    both = two_terms(load_ref[...])
    iload = jnp.zeros((8, 100), F32)
    for e in range(8):
        inverse = matrix(mid_inv, e, 100, 100, 33).astype(BF16)
        iload = jnp.where(row100 == e, times_transposed(both, inverse), iload)
        inner = matrix(mid_cif, e, 100, 200, 57).astype(BF16)
        imap_ref[e] = jnp.dot(inverse, inner, preferred_element_type=F32).astype(BF16)
    iload_ref[...] = iload
    both = two_terms(iload)
    outer_load = jnp.zeros((8, 200), F32)
    for e in range(8):
        outer = matrix(mid_cfi, e, 200, 100, 57).astype(BF16)
        outer_load = jnp.where(row200 == e, times_transposed(both, outer), outer_load)
        product = jnp.dot(outer, imap_ref[e], preferred_element_type=F32)
        alive = jnp.where(e < count, 1.0, 0.0)
        block = ((matrix(mid_ff, e, 200, 200, 105) - product) * alive).astype(BF16)
        condensed_ref[e] = block
        block = block.astype(F32)
        wide[0, 200 * e : 200 * e + 200, :] = block[:, 0:128]
        wide[1, 200 * e : 200 * e + 200, :] = jnp.concatenate([block[:, 128:200], jnp.zeros((200, 56), F32)], axis=1)
    face_load_ref[...] = jnp.where(row200 < count, fload_ref[...] - outer_load, 0.0)

    lane = lax.broadcasted_iota(jnp.int32, (8, 128), 1)
    for side in range(4):
        start = DOF * side
        tiles = [jnp.zeros((8, 128), F32) for _ in range(20)]
        for i in range(DOF):
            at = pl.ds(start + i, 8, stride=200)
            if side == 2:
                value = jnp.where(lane < 64, wide[1, at, :], wide[0, at, :])
            else:
                value = wide[start // 128, at, :]
            tile, off = divmod(DOF * i, 128)
            shift = (off - start) % 128
            value = pltpu.roll(value, shift, 1) if shift else value
            tiles[tile] = jnp.where((lane >= off) & (lane < off + DOF), value, tiles[tile])
            if off + DOF > 128:
                tiles[tile + 1] = jnp.where(lane < off + DOF - 128, value, tiles[tile + 1])
        blocks_ref[8 * side : 8 * side + 8, :] = jnp.concatenate(tiles, axis=1).astype(BF16)


def slots_of(wide):
    lane = lax.broadcasted_iota(jnp.int32, (8, 128), 1)
    pieces = []
    for side in range(4):
        turned = wide if side == 0 else pltpu.roll(wide, 256 - DOF * side, 1)
        pieces.append(jnp.where(lane < DOF, turned[:, 0:128], 0.0))
    return jnp.concatenate(pieces, axis=0)


def elements_of(slots):
    zero = jnp.zeros((8, 128), F32)
    total = jnp.concatenate([slots[0:8], zero], axis=1)
    for side in range(1, 4):
        wide = jnp.concatenate([slots[8 * side : 8 * side + 8], zero], axis=1)
        total = total + pltpu.roll(wide, DOF * side, 1)
    return total


def each_element(elements, matrix_ref, rows):
    both = two_terms(elements)[:, 0:200]
    row = lax.broadcasted_iota(jnp.int32, (8, rows), 0)
    total = jnp.zeros((8, rows), F32)
    for e in range(8):
        total = jnp.where(row == e, times_transposed(both, matrix_ref[e]), total)
    return total


def twice(rows):
    return jnp.concatenate([rows, pltpu.roll(rows, 64, 1)], axis=0)


MIRROR = (0, 3, 2, 1)


def virtual_hots(slot_ref, send_ref, recv_ref, partner_ref, subs):
    lane = lax.broadcasted_iota(jnp.int32, (8, 128), 1)
    row = lax.broadcasted_iota(jnp.int32, (8, 128), 0)
    row24 = lax.broadcasted_iota(jnp.int32, (24, 128), 0)
    row32 = lax.broadcasted_iota(jnp.int32, (32, 128), 0)
    nothing = jnp.full((8, 128), -1000, jnp.int32)
    no = jnp.zeros((8, 128), F32)
    faces, slots = {}, {}
    for g in range(GROUPS):
        for r in range(2):
            face, slot = recv_ref[0, r, g], send_ref[0, r, g]
            faces[g, r] = jnp.where(face < 24, face, -1000)
            slots[g, r] = jnp.where(slot < 32, (slot & 3) * 8 + (slot >> 2), -1000)
    table_l, columns = nothing, []
    for side in range(4):
        column = nothing
        for e in range(8):
            face = slot_ref[side, e]
            face = jnp.where(face < 24, face, -1000)
            table_l = jnp.where(lane == 8 * side + e, face, table_l)
            column = jnp.where(row == e, face, column)
        columns.append(column)
    table_e, table_d, table_f = nothing, nothing, nothing
    hot_g, hot_r, hot_j, pick = no, no, no, [no, no]
    for g in range(GROUPS):
        holder, owner = partner_ref[0, g], partner_ref[0, GROUPS + g]
        mirror = MIRROR[g]
        for r in range(2):
            face, slot, rank = faces[g, r], slots[g, r], 24 + 2 * g + r
            table_l = jnp.where(lane == slot, rank, table_l)
            columns = [jnp.where(row + 8 * side == slot, rank, column) for side, column in enumerate(columns)]
            alive = jnp.where(slot >= 0, rank, -1000)
            table_e = jnp.where(lane == 64 * r + 2 * (subs * g + owner), alive, table_e)
            table_e = jnp.where(lane == 64 * r + 2 * (subs * mirror + holder) + 1, face, table_e)
            table_d = jnp.where(lane == 32 * r + subs * g + owner, alive, table_d)
            table_f = jnp.where(lane == 2 * g + r, face, table_f)
            hot_g = jnp.where((row == g) & (lane == 24 * r + face), 1.0, hot_g)
            hot_r = jnp.where((row == 2 * g + r) & (lane == slot), 1.0, hot_r)
            hot_j = jnp.where((row == 2 * g + r) & (lane == face), 1.0, hot_j)
            pick[r] = jnp.where((row == 2 * g) & (lane == face), 1.0, pick[r])
            pick[r] = jnp.where((row == 2 * mirror + 1) & (lane == rank), 1.0, pick[r])

    def equal(rows, table):
        return (rows == jnp.concatenate([table] * (rows.shape[0] // 8), axis=0)).astype(F32)

    hot_x = jnp.concatenate([(lane == column).astype(F32) for column in columns], axis=0)
    local = equal(row32, table_l).astype(BF16)
    sent = [jnp.dot(part.astype(BF16)[:, 0:32], local, preferred_element_type=F32) for part in pick]
    hot_s = sent[0] + pltpu.roll(sent[1], 32, 1)
    twins = jnp.int32(0)
    flat = [faces[g, r] for g in range(GROUPS) for r in range(2)]
    for k, face in enumerate(flat):
        for other in flat[:k]:
            twins = twins + jnp.where(face == other, jnp.where(face >= 0, 1, 0), 0)
    hots = (hot_s, hot_x, equal(row32, table_e), equal(row32, table_d), hot_g, hot_r, hot_j, equal(row24, table_f))
    return (local,) + tuple(hot.astype(BF16) for hot in hots) + (twins,)


def sweep_kernel(
    doms, subs,
    slot_hbm, send_hbm, recv_hbm, partner_hbm, count_hbm,
    inv_hbm, cif_hbm, cfi_hbm, ff_hbm, load_hbm, fload_hbm, jac_hbm,
    trace_ref, state_ref, faces_ref, twins_ref,
    jflat, jrows, esend, ebuf, dsend, dbuf, fsend, fbuf, bsend, bbuf, jsend, jbuf,
    esend_sem, erecv_sem, dsend_sem, drecv_sem, fsend_sem, frecv_sem, bsend_sem, brecv_sem, jsend_sem, jrecv_sem,
    inv_ref, cif_ref, cfi_ref, ff_ref, load_ref, fload_ref, jac_ref,
    slot_ref, send_ref, recv_ref, partner_ref, count_ref, in_sem,
    condensed_ref, imap_ref, iload_ref, face_load_ref, blocks_ref,
    *spaces,
):
    dom, sub = lax.axis_index("dom"), lax.axis_index("sub")
    mesh_ids = pl.DeviceIdType.MESH
    offsets = [group_offset(g, doms) for g in range(GROUPS)]
    barrier = pltpu.get_barrier_semaphore()
    rank, block = lax.rem(dom, 8), dom // 8

    def hello(target, other):
        pl.semaphore_signal(barrier, inc=1, device_id=(target, other), device_id_type=mesh_ids)

    def to_all(start):
        def body(step, carry):
            other = lax.rem(sub + far_first(step), subs)
            for g in (2, 1, 3, 0):
                target = lax.rem(dom + offsets[g], doms)
                if g == 0:
                    pl.when(step < subs - 1)(functools.partial(start, g, target, other))
                else:
                    start(g, target, other)
            return carry

        lax.fori_loop(0, subs, body, 0)

    stages = (
        lambda step: (dom, lax.rem(sub + step, subs)),
        lambda step: (lax.rem(dom + 8 * step, doms), sub),
        lambda step: (8 * block + lax.rem(rank + step, 8), sub),
    )
    places = (sub, block, rank)
    for phase in range(3):
        ebuf[phase] = jnp.zeros(ebuf.shape[1:], F32)
        fbuf[phase] = jnp.zeros(fbuf.shape[1:], F32)
    dbuf[...] = jnp.zeros(dbuf.shape, F32)
    to_all(lambda g, target, other: hello(target, other))

    def more(step, carry):
        hello(*stages[1](step))
        hello(*stages[2](step))
        return carry

    lax.fori_loop(1, 8, more, 0)
    loads = [
        pltpu.make_async_copy(source, target, in_sem.at[k])
        for k, (source, target) in enumerate(
            (
                (inv_hbm, inv_ref), (cfi_hbm, cfi_ref), (cif_hbm, cif_ref), (ff_hbm, ff_ref),
                (load_hbm, load_ref), (fload_hbm, fload_ref), (jac_hbm, jac_ref),
                (slot_hbm, slot_ref), (send_hbm, send_ref), (recv_hbm, recv_ref),
                (partner_hbm, partner_ref), (count_hbm, count_ref),
            )
        )
    ]
    for load in loads:
        load.start()
    condense_body(
        loads, inv_ref, cif_ref, cfi_ref, ff_ref, load_ref, fload_ref, count_ref,
        condensed_ref, imap_ref, iload_ref, face_load_ref, blocks_ref, *spaces,
    )
    local, hot_s, hot_x, hot_e, hot_d, hot_g, hot_r, hot_j, hot_f, twins = virtual_hots(
        slot_ref, send_ref, recv_ref, partner_ref, subs
    )

    def fill_rows(first, rows):
        for i in range(DOF):
            start = DOF * i
            base = min(start // 128 * 128, 2432)
            window = jflat[first : first + rows, base : base + 256]
            jrows[i, first : first + rows, :] = pltpu.roll(window, 256 - (start - base), 1)[:, 0:128]

    loads[6].wait()
    jflat[0:24, 0:2500] = jac_ref[...].astype(F32)
    jflat[:, 2500:2688] = jnp.zeros((32, 188), F32)
    jflat[24:32, 0:2500] = jnp.zeros((8, 2500), F32)
    for i in range(DOF):
        jrows[i, 24:32, :] = jnp.zeros((8, 128), F32)
    fill_rows(0, 24)
    part = 2560 // CHUNKS
    inverses = jflat[0:24, 0:2560].astype(BF16)
    blocks = blocks_ref[...]
    picked_j = jnp.dot(hot_j[:, 0:24], inverses, preferred_element_type=F32)
    picked_b = jnp.dot(hot_r[:, 0:32], blocks, preferred_element_type=F32)
    for chunk in range(CHUNKS):
        for g in range(GROUPS):
            jsend[chunk, g] = picked_j[2 * g : 2 * g + 2, chunk * part : (chunk + 1) * part]
            bsend[chunk, MIRROR[g]] = picked_b[2 * g : 2 * g + 2, chunk * part : (chunk + 1) * part]
    lane32 = lax.broadcasted_iota(jnp.int32, (32, 128), 1)

    def short(rows):
        return jnp.where(lane32 < DOF, rows, 0.0)

    def jacobi(vector):
        total = jnp.zeros((32, 128), F32)
        for i in range(DOF):
            entry = jnp.sum(jrows[i] * vector, axis=1, keepdims=True)
            total = jnp.where(lane32 == i, entry, total)
        return total

    def start_swap(phase, slots):
        esend[phase] = split_dot(hot_s[:, 0:64], twice(slots))

        def start(g, target, other):
            pltpu.make_async_remote_copy(
                src_ref=esend.at[phase, pl.ds(2 * g, 2)],
                dst_ref=ebuf.at[phase, pl.ds(2 * (g * subs + sub), 2)],
                send_sem=esend_sem.at[phase], recv_sem=erecv_sem.at[phase],
                device_id=(target, other), device_id_type=mesh_ids,
            ).start()

        to_all(start)

    def finish_swap(phase, slots):
        own = split_dot(local[:, 0:32], slots)
        whole = ebuf.at[phase, pl.ds(0, 62)]
        pltpu.make_async_copy(whole, whole, erecv_sem.at[phase]).wait()
        return short(own + split_dot(hot_e, twice(ebuf[phase])))

    def start_stage(stage, value):
        fsend[stage] = value

        def body(step, carry):
            pltpu.make_async_remote_copy(
                src_ref=fsend.at[stage, pl.ds(0, 1)], dst_ref=fbuf.at[stage, pl.ds(places[stage], 1)],
                send_sem=fsend_sem.at[stage], recv_sem=frecv_sem.at[stage],
                device_id=stages[stage](step), device_id_type=mesh_ids,
            ).start()
            return carry

        lax.fori_loop(1, 8, body, 0)

    def finish_stage(stage, value):
        whole = fbuf.at[stage, pl.ds(0, 7)]
        pltpu.make_async_copy(whole, whole, frecv_sem.at[stage]).wait()
        return value + jnp.sum(fbuf[stage], axis=0, keepdims=True)

    def start_chunks(source, target_ref, send_sem, recv_sem, first, last):
        for chunk in range(first, last):

            def start(g, target, other):
                pltpu.make_async_remote_copy(
                    src_ref=source.at[chunk, g], dst_ref=target_ref.at[chunk, g * subs + sub],
                    send_sem=send_sem.at[chunk], recv_sem=recv_sem.at[chunk],
                    device_id=(target, other), device_id_type=mesh_ids,
                ).start()

            to_all(start)

    def finish_chunks(target_ref, recv_sem, index):
        for chunk in range(CHUNKS):
            whole = target_ref.at[chunk, pl.ds(0, 31)]
            pltpu.make_async_copy(whole, whole, recv_sem.at[chunk]).wait()
        rows = [
            jnp.concatenate([target_ref[chunk, index(g)] for chunk in range(CHUNKS)], axis=1) for g in range(GROUPS)
        ]
        return jnp.concatenate(rows, axis=0)

    start_jac = functools.partial(start_chunks, jsend, jbuf, jsend_sem, jrecv_sem)
    start_blocks = functools.partial(start_chunks, bsend, bbuf, bsend_sem, brecv_sem)
    found = jnp.zeros((8, 128), F32) + twins.astype(F32)

    def padded(rows):
        return jnp.concatenate([rows, jnp.zeros((8, 56), F32)], axis=1)

    slots = slots_of(padded(face_load_ref[...]))
    pl.semaphore_wait(barrier, 45)
    start_swap(0, slots)
    start_stage(0, found)
    start_jac(0, 3)
    rhs = finish_swap(0, slots)
    found = finish_stage(0, found)
    traces = jacobi(rhs)

    dsend[...] = split_dot(hot_g[:, 0:48], twice(traces[0:24]))

    def start_trace(g, target, other):
        pltpu.make_async_remote_copy(
            src_ref=dsend.at[pl.ds(g, 1)], dst_ref=dbuf.at[pl.ds(g * subs + sub, 1)],
            send_sem=dsend_sem, recv_sem=drecv_sem, device_id=(target, other), device_id_type=mesh_ids,
        ).start()

    to_all(start_trace)
    start_stage(1, found)
    start_jac(3, 5)
    start_blocks(0, 1)
    pltpu.make_async_copy(dbuf.at[pl.ds(0, 31)], dbuf.at[pl.ds(0, 31)], drecv_sem).wait()
    traces = short(traces + split_dot(hot_d[:, 0:64], twice(dbuf[...])))
    found = finish_stage(1, found)

    for sweep in range(SWEEPS):
        elements = elements_of(short(split_dot(hot_x[:, 0:32], traces)))
        slots = slots_of(padded(each_element(elements, condensed_ref, 200)))
        start_swap(1 + sweep, slots)
        if sweep == 0:
            start_blocks(1, 4)
        else:
            start_blocks(4, 5)
        if sweep == 0:
            start_stage(2, found)
        total = finish_swap(1 + sweep, slots)
        if sweep == 0:
            jflat[24:32, 0:2560] = finish_chunks(jbuf, jrecv_sem, lambda g: g * subs + partner_ref[0, GROUPS + g])
            fill_rows(24, 8)
        traces = traces + jacobi(rhs - total)
    twins_ref[...] = jnp.where(finish_stage(2, found)[0:1, 0:1] > 0.0, 1, 0)
    trace_ref[...] = traces[0:24]
    elements = elements_of(short(split_dot(hot_x[:, 0:32], traces)))
    row100 = lax.broadcasted_iota(jnp.int32, (8, 100), 0)
    state = iload_ref[...] - each_element(elements, imap_ref, 100)
    state = jnp.where(row100 < count_ref[0], state, 0.0)
    state_ref[...] = jnp.concatenate([state, jnp.zeros((8, 28), F32)], axis=1)
    sums = jnp.dot(local[0:24, 0:32], blocks, preferred_element_type=F32)
    far = finish_chunks(bbuf, brecv_sem, lambda g: MIRROR[g] * subs + partner_ref[0, g]).astype(BF16)
    faces_ref[...] = sums + jnp.dot(hot_f[:, 0:8], far, preferred_element_type=F32)
    for phase in range(3):
        pltpu.make_async_copy(ebuf.at[phase, pl.ds(0, 62)], ebuf.at[phase, pl.ds(0, 62)], esend_sem.at[phase]).wait()
        pltpu.make_async_copy(fbuf.at[phase, pl.ds(0, 7)], fbuf.at[phase, pl.ds(0, 7)], fsend_sem.at[phase]).wait()
    pltpu.make_async_copy(dbuf.at[pl.ds(0, 31)], dbuf.at[pl.ds(0, 31)], dsend_sem).wait()
    for chunk in range(CHUNKS):
        whole = bbuf.at[chunk, pl.ds(0, 31)]
        pltpu.make_async_copy(whole, whole, bsend_sem.at[chunk]).wait()
        whole = jbuf.at[chunk, pl.ds(0, 31)]
        pltpu.make_async_copy(whole, whole, jsend_sem.at[chunk]).wait()


def finish_kernel(trace_ref, state_ref, faces_ref, trace_out, state_out, faces_out):
    trace_out[...] = trace_ref[:, 0:DOF]
    state_out[...] = state_ref[:, 0:100]
    faces_out[...] = faces_ref[:, 0 : DOF * DOF].astype(BF16)


def six_exchanges(
    doms, subs,
    inv_interior, couple_if, couple_fi, face_face, load_interior, load_face, jacobi_inverse,
    slot_face, send_slot, recv_face, partner_sub, elem_count,
):
    vmem = pl.BlockSpec(memory_space=pltpu.VMEM)
    part = 2560 // CHUNKS
    results = pl.pallas_call(
        functools.partial(exchange_kernel, doms, subs),
        out_shape=(
            jax.ShapeDtypeStruct((24, 128), F32),
            jax.ShapeDtypeStruct((8, 128), F32),
            jax.ShapeDtypeStruct((24, 2560), F32),
        ),
        in_specs=[pl.BlockSpec(memory_space=pl.ANY)] * 12,
        out_specs=(vmem, vmem, vmem),
        scratch_shapes=[
            pltpu.VMEM((24, 2688), F32),
            pltpu.VMEM((DOF, 24, 128), F32),
            pltpu.VMEM((6, 8, 128), F32),
            pltpu.VMEM((6, 32, 128), F32),
            pltpu.VMEM((CHUNKS, GROUPS, 2, part), F32),
            pltpu.VMEM((CHUNKS, 32, 2, part), F32),
            pltpu.SemaphoreType.DMA((6,)),
            pltpu.SemaphoreType.DMA((6,)),
            pltpu.SemaphoreType.DMA((CHUNKS,)),
            pltpu.SemaphoreType.DMA((CHUNKS,)),
        ] + local_scratch(inv_interior, couple_if, couple_fi, face_face),
        compiler_params=pltpu.CompilerParams(collective_id=1, has_side_effects=True),
    )(
        slot_face.T, send_slot.transpose(0, 2, 1), recv_face.transpose(0, 2, 1), partner_sub, elem_count,
        inv_interior, couple_if, couple_fi, face_face, load_interior, load_face, jacobi_inverse,
    )
    return finish(results)


def local_scratch(inv_interior, couple_if, couple_fi, face_face):
    return [
        pltpu.VMEM(inv_interior.shape, BF16),
        pltpu.VMEM(couple_if.shape, BF16),
        pltpu.VMEM(couple_fi.shape, BF16),
        pltpu.VMEM(face_face.shape, BF16),
        pltpu.VMEM((8, 100), F32),
        pltpu.VMEM((8, 200), F32),
        pltpu.VMEM((24, 2500), BF16),
        pltpu.SMEM((4, 8), jnp.int32),
        pltpu.SMEM((1, 2, 4), jnp.int32),
        pltpu.SMEM((1, 2, 4), jnp.int32),
        pltpu.SMEM((1, 8), jnp.int32),
        pltpu.SMEM((1,), jnp.int32),
        pltpu.SemaphoreType.DMA((12,)),
        pltpu.VMEM((8, 200, 200), BF16),
        pltpu.VMEM((8, 100, 200), BF16),
        pltpu.VMEM((8, 100), F32),
        pltpu.VMEM((8, 200), F32),
        pltpu.VMEM((32, 2560), BF16),
        pltpu.VMEM((808, 128), F32),
        pltpu.VMEM((1408, 128), F32),
        pltpu.VMEM((1408, 128), F32),
        pltpu.VMEM((2608, 128), F32),
        pltpu.VMEM((1, 1064, 128), F32),
        pltpu.VMEM((2, 920, 128), F32),
        pltpu.VMEM((1, 1832, 128), F32),
        pltpu.VMEM((2, 1688, 128), F32),
        pltpu.VMEM((2, 1600, 128), F32),
    ]


def finish(results):
    vmem = pl.BlockSpec(memory_space=pltpu.VMEM)
    return pl.pallas_call(
        finish_kernel,
        out_shape=(
            jax.ShapeDtypeStruct((24, DOF), F32),
            jax.ShapeDtypeStruct((8, 100), F32),
            jax.ShapeDtypeStruct((24, DOF * DOF), BF16),
        ),
        in_specs=[vmem] * 3,
        out_specs=(vmem, vmem, vmem),
    )(*results)


def per_device(doms, subs, *arrays):
    vmem = pl.BlockSpec(memory_space=pltpu.VMEM)
    part = 2560 // CHUNKS
    loads, tables = arrays[:7], arrays[7:]
    slot_face, send_slot, recv_face, partner_sub, elem_count = tables
    *results, twins = pl.pallas_call(
        functools.partial(sweep_kernel, doms, subs),
        out_shape=(
            jax.ShapeDtypeStruct((24, 128), F32),
            jax.ShapeDtypeStruct((8, 128), F32),
            jax.ShapeDtypeStruct((24, 2560), F32),
            jax.ShapeDtypeStruct((1, 1), jnp.int32),
        ),
        in_specs=[pl.BlockSpec(memory_space=pl.ANY)] * 12,
        out_specs=(vmem, vmem, vmem, vmem),
        scratch_shapes=[
            pltpu.VMEM((32, 2688), F32),
            pltpu.VMEM((DOF, 32, 128), F32),
            pltpu.VMEM((3, 8, 128), F32),
            pltpu.VMEM((3, 64, 128), F32),
            pltpu.VMEM((8, 128), F32),
            pltpu.VMEM((32, 128), F32),
            pltpu.VMEM((3, 8, 128), F32),
            pltpu.VMEM((3, 8, 128), F32),
            pltpu.VMEM((CHUNKS, GROUPS, 2, part), F32),
            pltpu.VMEM((CHUNKS, 32, 2, part), F32),
            pltpu.VMEM((CHUNKS, GROUPS, 2, part), F32),
            pltpu.VMEM((CHUNKS, 32, 2, part), F32),
            pltpu.SemaphoreType.DMA((3,)),
            pltpu.SemaphoreType.DMA((3,)),
            pltpu.SemaphoreType.DMA,
            pltpu.SemaphoreType.DMA,
            pltpu.SemaphoreType.DMA((3,)),
            pltpu.SemaphoreType.DMA((3,)),
            pltpu.SemaphoreType.DMA((CHUNKS,)),
            pltpu.SemaphoreType.DMA((CHUNKS,)),
            pltpu.SemaphoreType.DMA((CHUNKS,)),
            pltpu.SemaphoreType.DMA((CHUNKS,)),
        ] + local_scratch(*loads[:4]),
        compiler_params=pltpu.CompilerParams(collective_id=0, has_side_effects=True, vmem_limit_bytes=67043328),
    )(slot_face.T, send_slot.transpose(0, 2, 1), recv_face.transpose(0, 2, 1), partner_sub, elem_count, *loads)
    return lax.switch(
        twins.reshape(()),
        (lambda: finish(results), lambda: six_exchanges(doms, subs, *arrays)),
    )


def solution(mesh):
    rows = P(("dom", "sub"), None)
    placed = (rows,) * 8 + (P(("dom", "sub"), None, None),) * 2 + (rows, P(("dom", "sub")))
    return jax.shard_map(
        functools.partial(per_device, mesh.shape["dom"], mesh.shape["sub"]),
        mesh=mesh,
        in_specs=placed,
        out_specs=(rows, rows, rows),
        check_vma=False,
    )
```
